256 devices in a mesh: dp: 32 (over y, x, core), mp: 8 (over z).
Axes of the slice: x: 4, y: 4, z: 8, core: 2. Of those that a mesh axis runs over, the one named last changes fastest.
Arguments:
- grad_out: bfloat16 [4096, 2688], P('dp', 'mp'), may hold values from -24 to 24
- gate_pre: bfloat16 [4096, 10752], P('dp', 'mp'), may hold values from -6 to 6
- up_pre: bfloat16 [4096, 10752], P('dp', 'mp'), may hold values from -6 to 6
- down_weight: bfloat16 [2688, 10752], P('dp', 'mp'), may hold values from -0.125 to 0.125
- new_logp: float32 [4096], P('dp'), may hold values from -3 to 0
- behav_logp: float32 [4096], P('dp'), may hold values from -3 to 0
- lengths: int32 [32], P('dp'), may hold values from 1 to 128
- versions: int32 [32], P('dp'), may hold values from 0 to 7
- token_lag: int32 [4096], P('dp'), may hold values from 0 to 3
Outputs:
- d_gate: bfloat16 [4096, 10752], P('dp', 'mp')
- d_up: bfloat16 [4096, 10752], P('dp', 'mp')
- d_down: float32 [2688, 10752], P('dp', 'mp')
The draws below stay inside these ranges and needn't reach their ends.
All inputs are finite; a program needn't handle non-finite values.
Results may differ from the reference program's by a relative error of at most 0.017.
Values may be sent and summed in bfloat16 or wider, within the bound.
A program may use at most 64 MiB of HBM per device.

```python
import jax
import jax.numpy as jnp
from jax import lax

D = 2688
FF = 10752
LEN = 128
SEQ_DEV = 1
VERSIONS = 8
LAGS = 4
MAX_LAG = 5
TOK_DEV = 128
SEQS = 32
TOKENS = 4096


def draw_lengths(key, part):
    seq_index = jnp.arange(SEQS, dtype=jnp.int32)
    groups = SEQS // SEQ_DEV
    spread = max(groups - 1, 1)
    device = seq_index // SEQ_DEV
    highest = LEN * (spread + 2 * device) // (3 * spread)
    highest = jnp.maximum(highest, 2)
    lowest = highest // 2
    random_bits = jax.random.randint(key, (SEQS,), 0, 1 << 20)
    length = lowest + random_bits % (highest - lowest + 1)
    length = jnp.where(seq_index == SEQS - 1, LEN, length)
    return jnp.clip(length, 1, LEN).astype(jnp.int32)


def place_ends(array, stream_key, low, largest):
    shape = array.shape
    place = [jax.random.randint(jax.random.fold_in(stream_key, axis), (), 0, shape[axis]) for axis in range(len(shape))]
    array = array.at[tuple(place)].set(low)
    longest = shape.index(max(shape))
    place[longest] = (place[longest] + 1) % shape[longest]
    return array.at[tuple(place)].set(largest)


def strengthened(entries, rng, source, target, blocks, factor):
    owner, partner = [(jnp.arange(entries.shape[axis_at]) // (entries.shape[axis_at] // blocks)).reshape([-1 if axis == axis_at else 1 for axis in range(entries.ndim)]) for axis_at in (source, target)]
    chosen = jax.random.permutation(rng, blocks)[partner]
    strong = (owner == chosen) | (owner == (partner + blocks // 2) % blocks)
    return jnp.where(strong, factor * entries, entries)


def block_scale(own_key, dims, pieces, low, high):
    gain, own = 1.0, jax.random.fold_in(own_key, 6)
    for dim, blocks in pieces:
        steps = jnp.exp(jax.random.uniform(jax.random.fold_in(own, dim), (blocks,), jnp.float32, low / len(pieces), high / len(pieces)))
        gain = gain * jnp.repeat(steps, dims[dim] // blocks).reshape([-1 if axis == dim else 1 for axis in range(len(dims))])
    return gain


def normal_values(stream_key, shape, deviation, limit, shards=(), kind=jnp.bfloat16):
    array = deviation * jax.random.normal(stream_key, shape, jnp.float32)
    if shards:
        array = array * block_scale(stream_key, shape, shards, -0.22, 0.18)
    return jnp.clip(array, -limit, limit).astype(kind)


def noise_with(key, shape, width, most, shards, heavy, kind=jnp.bfloat16):
    result = width * jax.random.normal(key, shape, jnp.float32)
    if shards:
        result = result * block_scale(key, shape, shards, -0.22, 0.18)
    return jnp.clip(strengthened(result, jax.random.fold_in(key, 3), *heavy), -most, most).astype(kind)


def setup_inputs(seed: int = 0) -> dict:
    arg_keys = jax.random.split(jax.random.key(seed), 10)
    return {
        "grad_out": noise_with(arg_keys[0], (TOKENS, D), 4.0, 24.0, ((0, 32), (1, 8)), (0, 1, 32, 2.75)),
        "gate_pre": normal_values(arg_keys[1], (TOKENS, FF), 1.0, 6.0, ((0, 32), (1, 8))),
        "up_pre": normal_values(arg_keys[2], (TOKENS, FF), 1.0, 6.0, ((0, 32), (1, 8))),
        "down_weight": normal_values(arg_keys[3], (D, FF), D ** -0.5, 0.125, ((0, 32), (1, 8))),
        "new_logp": jnp.clip(-3.0 + 3.0 * jax.random.uniform(arg_keys[4], (TOKENS,), jnp.float32) ** block_scale(arg_keys[4], (TOKENS,), ((0, 32),), -0.2, 0.2), -3.0, 0.0),
        "behav_logp": jnp.clip(-3.0 + 3.0 * jax.random.uniform(arg_keys[5], (TOKENS,), jnp.float32) ** block_scale(arg_keys[5], (TOKENS,), ((0, 32),), -0.2, 0.2), -3.0, 0.0),
        "lengths": draw_lengths(jax.random.fold_in(arg_keys[9], 71), 0),
        "versions": place_ends(jax.random.randint(arg_keys[7], (SEQS,), 0, VERSIONS), jax.random.fold_in(arg_keys[7], 1), 0, VERSIONS - 1).astype(jnp.int32),
        "token_lag": place_ends(jax.random.randint(arg_keys[8], (TOKENS,), 0, LAGS), jax.random.fold_in(arg_keys[8], 1), 0, LAGS - 1).astype(jnp.int32),
    }


ratio_cap = 2.0


def gelu_tanh(values):
    return jax.nn.gelu(values, approximate=True)


def reference(grad_out, gate_pre, up_pre, down_weight, new_logp, behav_logp, lengths, versions, token_lag):
    token_ids = jnp.arange(TOKENS, dtype=jnp.int32)
    positions = token_ids % LEN
    seq_of = token_ids // LEN
    in_length = positions < lengths[seq_of]
    token_version = versions[seq_of] + token_lag
    current = jnp.max(jnp.where(in_length, token_version, -1))
    is_valid = in_length & (token_version >= current - MAX_LAG)
    valid_count = jnp.sum(is_valid.astype(jnp.float32))
    ratios = jnp.minimum(jnp.exp(new_logp - behav_logp), ratio_cap)
    weights = jnp.where(is_valid, ratios, jnp.float32(0.0)) * (SEQS / valid_count)
    scaled = (weights[:, None] * grad_out.astype(jnp.float32)).astype(jnp.bfloat16)
    gate = gate_pre.astype(jnp.float32)
    upper = up_pre.astype(jnp.float32)
    activated, slope = jax.jvp(gelu_tanh, (gate,), (jnp.ones_like(gate),))
    hidden = (activated * upper).astype(jnp.bfloat16)
    blocks = SEQS // SEQ_DEV
    scaled_blocks = scaled.reshape(blocks, TOK_DEV, D)
    hidden_blocks = hidden.reshape(blocks, TOK_DEV, FF)

    def add_block(total, pair):
        partial_sum = lax.dot_general(pair[0], pair[1], (((0,), (0,)), ((), ())), preferred_element_type=jnp.float32)
        rounded = lax.optimization_barrier(partial_sum.astype(jnp.bfloat16))
        return total + rounded.astype(jnp.float32), None

    d_down, unused = lax.scan(add_block, jnp.zeros((D, FF), jnp.float32), (scaled_blocks, hidden_blocks))
    d_hidden = jnp.dot(scaled, down_weight, preferred_element_type=jnp.float32)
    d_up = (d_hidden * activated).astype(jnp.bfloat16)
    d_gate = (d_hidden * upper * slope).astype(jnp.bfloat16)
    return d_gate, d_up, d_down
```

```python
import functools
import math

import jax
import jax.numpy as jnp
from jax import lax
from jax.experimental import pallas as pl
from jax.experimental.pallas import tpu as pltpu
from jax.sharding import Mesh
from jax.sharding import PartitionSpec as P

MAX_LAG = 5
DP = ("dp_0", "dp_1", "dp_2")
MESH = pl.DeviceIdType.MESH
F32, BF16 = jnp.float32, jnp.bfloat16
RATIO_CAP = 2.0
ROOT = math.sqrt(2.0 / math.pi)
CUBIC = 0.044715


def kernel(
    rows, low, weight, cotangent, gate, up, new_logp, old_logp, lag, length, version,
    d_gate, d_up, d_down,
    weights_all, cot_all, cot_mine, hidden, gate_v, up_v, act, up_slope, parts, others, acc, acc_in, hist_out, hist_in,
    partial, far_out, full_out, half_in, full_in, far_out1, full_out1, half_in1, full_in1, gate_out, up_out, down_out,
    copy_sem, out_sem, hist_send, hist_recv, z_send, z_recv, ag_send, ag_recv, core_send, core_recv,
    a_send, f_send, h_recv, f_recv, a1_send, f1_send, h1_recv, f1_recv,
):
    y, x, c, z = (lax.axis_index(name) for name in (*DP, "mp"))
    tokens = hidden.shape[0] // 2
    lo, hi = pl.ds(0, low), pl.ds(low, rows - low)

    def at(i, j):
        return (
            lax.rem(y + 4 + i * c + j * (1 - c), 4),
            lax.rem(x + 4 + i * (1 - c) + j * c, 4),
        )

    def device(i, j):
        yy, xx = at(i, j)
        return (yy, xx, c, z)

    def block(i, j):
        yy, xx = at(i, j)
        return yy * 4 + xx

    twin = (y, x, 1 - c, z)
    z_peers = [(y, x, c, lax.rem(z + d, 8)) for d in range(1, 8)]
    x_peers = [(y, lax.rem(x + d, 4), c, z) for d in range(1, 4)]
    y_peers = [(lax.rem(y + d, 4), x, c, z) for d in range(1, 4)]
    peers = [twin, *z_peers, *x_peers, *y_peers]

    def remote(src, dst, send, recv, to):
        return pltpu.make_async_remote_copy(
            src_ref=src, dst_ref=dst, send_sem=send, recv_sem=recv, device_id=to, device_id_type=MESH
        )

    barrier = pltpu.get_barrier_semaphore()
    for peer in peers:
        pl.semaphore_signal(barrier, inc=1, device_id=peer, device_id_type=MESH)

    own = block(0, 0)
    local = [
        pltpu.make_async_copy(gate, gate_v, copy_sem.at[0]),
        pltpu.make_async_copy(up, up_v, copy_sem.at[1]),
        pltpu.make_async_copy(cotangent, cot_mine, copy_sem.at[2]),
        pltpu.make_async_copy(weight, weights_all.at[own], copy_sem.at[3]),
    ]
    for copy in local:
        copy.start()

    bins = lax.broadcasted_iota(jnp.int32, (16, tokens), 0)
    position = lax.broadcasted_iota(jnp.int32, (1, tokens), 1)
    live = position < length[0]
    token_version = lag[...] + version[0]
    match = jnp.where((token_version == bins) & live, 1.0, 0.0)
    counts = jnp.broadcast_to(jnp.sum(match, axis=1, keepdims=True), (16, tokens))
    hist_out[0] = counts

    pl.semaphore_wait(barrier, len(peers))

    sent = []

    def go(copy):
        copy.start()
        sent.append(copy)

    for d in range(3):
        go(remote(hist_out.at[0], hist_in.at[d], hist_send.at[d], hist_recv.at[d], x_peers[d]))

    fulls = {(-1, 0): 0, (1, 0): 1, (0, -1): 2, (0, 1): 3, (-1, -1): 4, (-1, 1): 5, (1, -1): 6, (1, 1): 7, (2, -1): 8, (2, 1): 9}
    halves = {(2, 0): 10, (0, 2): 12, (-1, 2): 14, (1, 2): 16, (2, 2): 18}
    steps = {0: (1, 0), 1: (-1, 0), 2: (0, 1), 3: (0, -1)}

    def forward(i, j, way, half=None, src=None):
        di, dj = steps[way]
        slot = weights_all.at[block(i, j)]
        ni, nj = i - di, j - dj
        if half is None:
            sem = fulls[(ni, nj)]
            part = slot
        else:
            ni, nj = (2 if ni in (-2, 2) else ni), (2 if nj in (-2, 2) else nj)
            sem = halves[(ni, nj)] + half
            part = slot.at[lo if half == 0 else hi]
        go(remote(part if src is None else src, part, ag_send.at[len(used)], ag_recv.at[sem], device(di, dj)))
        used.append(sem)

    used = []

    def landed(i, j, half=None):
        slot = weights_all.at[block(i, j)]
        if half is None:
            sem, part = fulls[(i, j)], slot
        else:
            sem, part = halves[(i, j)] + half, slot.at[lo if half == 0 else hi]
        remote(part, part, ag_send.at[0], ag_recv.at[sem], twin).wait_recv()

    for way in range(4):
        forward(0, 0, way, src=weight)
    for d in range(7):
        go(remote(cotangent, cot_all.at[d], z_send.at[d], z_recv.at[d], z_peers[d]))

    local[0].wait()
    local[1].wait()

    def elementwise(n, carry):
        at_rows = pl.ds(pl.multiple_of(n * 16, 16), 16)
        v = gate_v[at_rows].astype(F32)
        u = up_v[at_rows].astype(F32)
        square = v * v
        t = jnp.tanh(ROOT * (v + CUBIC * (square * v)))
        half = 0.5 * (1.0 + t)
        a = v * half
        slope = half + (0.5 * v) * (1.0 - t * t) * (ROOT * (1.0 + (3.0 * CUBIC) * square))
        act[at_rows] = a
        up_slope[at_rows] = u * slope
        hidden[at_rows] = (a * u).astype(BF16)
        return carry

    lax.fori_loop(0, tokens // 16, elementwise, 0)
    mine, theirs = pl.ds(0, tokens), pl.ds(tokens, tokens)
    swap_hidden = remote(hidden.at[mine], hidden.at[theirs], core_send.at[0], core_recv.at[0], twin)
    swap_hidden.start()

    def received(n):
        remote(hist_in.at[n], hist_in.at[n], hist_send.at[n], hist_recv.at[n], twin).wait_recv()
        return hist_in[n]

    counts = counts + received(0) + received(1) + received(2)
    hist_out[1] = counts
    for d in range(3):
        go(remote(hist_out.at[1], hist_in.at[3 + d], hist_send.at[3 + d], hist_recv.at[3 + d], y_peers[d]))

    for i in (-1, 1):
        landed(i, 0)
        forward(i, 0, 0 if i == -1 else 1, half=0 if i == -1 else 1)
        forward(i, 0, 2)
        forward(i, 0, 3)

    counts = counts + received(3) + received(4) + received(5)
    hist_out[2] = counts
    go(remote(hist_out.at[2], hist_in.at[6], hist_send.at[6], hist_recv.at[6], twin))

    def pass_on(i):
        landed(i, -1)
        forward(i, -1, 2, half=0)
        landed(i, 1)
        forward(i, 1, 3, half=1)

    pass_on(0)
    landed(2, 0, 0)
    landed(2, 0, 1)
    forward(2, 0, 2)
    forward(2, 0, 3)

    counts = counts + received(6)
    current = jnp.max(jnp.where(counts > 0, bins, -1), axis=0, keepdims=True)
    oldest = current - MAX_LAG
    valid_count = jnp.sum(jnp.where(bins >= oldest, counts, 0.0), axis=0, keepdims=True)
    valid = live & (token_version >= oldest)
    ratio = jnp.minimum(jnp.exp(new_logp[...] - old_logp[...]), RATIO_CAP)
    token_weight = jnp.where(valid, ratio, 0.0) * (32.0 / valid_count)
    row_id = lax.broadcasted_iota(jnp.int32, (tokens, tokens), 0)
    lane_id = lax.broadcasted_iota(jnp.int32, (tokens, tokens), 1)
    column = jnp.sum(jnp.where(row_id == lane_id, token_weight, 0.0), axis=1, keepdims=True)

    width = cotangent.shape[1]
    source = lax.broadcasted_iota(jnp.int32, (width, 512), 0)
    target = lax.broadcasted_iota(jnp.int32, (width, 512), 1)
    lane = target & 127
    group = target >> 7
    parity = jnp.where(group < 2, c, 1 - c)
    wanted = rows * (2 * (group & 1) + parity) + lane
    select = jnp.where((source == wanted) & (lane < rows), 1.0, 0.0).astype(BF16)

    def place(values, owner):
        scaled = (column * values.astype(F32)).astype(BF16)
        picked = jnp.dot(scaled, select, preferred_element_type=F32).astype(BF16)
        for k in range(2):
            parts[2 * owner + k, pl.ds(0, tokens), :] = picked[:, k * 128 : (k + 1) * 128]
            others[2 * owner + k] = picked[:, (k + 2) * 128 : (k + 3) * 128]

    local[2].wait()
    place(cot_mine[...], z)
    pass_on(-1)
    pass_on(1)

    def place_from(d, carry):
        remote(cot_all.at[d], cot_all.at[d], z_send.at[d], z_recv.at[d], twin).wait_recv()
        place(cot_all[d], lax.rem(z + 7 - d, 8))
        return carry

    lax.fori_loop(0, 7, place_from, 0)
    swap_parts = remote(others, parts.at[:, theirs], core_send.at[1], core_recv.at[1], twin)
    swap_parts.start()
    pass_on(2)
    swap_hidden.wait()
    swap_parts.wait_recv()

    def product(p):
        return lax.dot_general(
            parts[p], hidden[...], (((0,), (0,)), ((), ())), preferred_element_type=F32
        )[:rows]

    def offset(n):
        return jnp.where(n < 2, n + 2, 3 - n)

    def start_far(n, carry):
        far_out[n] = product(block(offset(n), 2)).astype(BF16)
        remote(far_out.at[n, lo], half_in.at[n, lo], a_send.at[n, 0], h_recv.at[n, 0], device(0, 1)).start()
        remote(far_out.at[n, hi], half_in.at[n, hi], a_send.at[n, 1], h_recv.at[n, 1], device(0, -1)).start()
        return carry

    lax.fori_loop(0, 4, start_far, 0)

    def rest(t, carry):
        n, m = t // 3, lax.rem(t, 3)
        partial[n, m] = product(block(offset(n), jnp.where(m == 0, 1, jnp.where(m == 1, 3, 0))))
        return carry

    lax.fori_loop(0, 12, rest, 0)

    for i in (0, -1, 1, 2):
        landed(i, 2, 0)
        landed(i, 2, 1)
    local[3].wait()
    acc[...] = jnp.zeros_like(acc)

    def accumulate(p, carry):
        acc[...] += jnp.dot(parts[p][:, :rows], weights_all[p], preferred_element_type=F32)
        return carry

    lax.fori_loop(0, 16, accumulate, 0)
    swap_acc = remote(acc.at[theirs], acc_in, core_send.at[2], core_recv.at[2], twin)
    swap_acc.start()

    def pass_full(n, carry):
        for side, (part, way) in enumerate(((lo, 1), (hi, -1))):
            remote(half_in.at[n, part], half_in.at[n, part], a_send.at[n, side], h_recv.at[n, side], twin).wait_recv()
            first = partial[n, side, lo]
            second = partial[n, side, hi]
            arrived = half_in[n, part].astype(F32)
            if side == 0:
                first = first + arrived
            else:
                second = second + arrived
            full_out[n, side, lo] = first.astype(BF16)
            full_out[n, side, hi] = second.astype(BF16)
            remote(full_out.at[n, side], full_in.at[n, side], f_send.at[n, side], f_recv.at[n, side], device(0, way)).start()
        return carry

    lax.fori_loop(0, 4, pass_full, 0)

    swap_acc.wait_recv()
    outs = []

    def finish(n, carry):
        at_rows = pl.ds(pl.multiple_of(n * 16, 16), 16)
        total = acc[at_rows] + acc_in[at_rows]
        up_out[at_rows] = (total * act[at_rows]).astype(BF16)
        gate_out[at_rows] = (total * up_slope[at_rows]).astype(BF16)
        return carry

    lax.fori_loop(0, tokens // 16, finish, 0)
    for n, (src, dst) in enumerate(((gate_out, d_gate), (up_out, d_up))):
        outs.append(pltpu.make_async_copy(src, dst, out_sem.at[n]))
        outs[-1].start()

    def ring_sum(n):
        for side in range(2):
            remote(full_in.at[n, side], full_in.at[n, side], f_send.at[n, side], f_recv.at[n, side], twin).wait_recv()
        return partial[n, 2] + full_in[n, 0].astype(F32) + full_in[n, 1].astype(F32)

    far_out1[...] = ring_sum(0).astype(BF16)
    far = [
        remote(far_out1.at[part], half_in1.at[part], a1_send.at[side], h1_recv.at[side], device(way, 0))
        for side, (part, way) in enumerate(((lo, 1), (hi, -1)))
    ]
    for copy in far:
        copy.start()
    full1 = []
    for n, side in ((1, 1), (2, 0)):
        down_out[...] = ring_sum(n)
        part, way = ((lo, 1), (hi, -1))[side]
        far[side].wait_recv()
        down_out[part] += half_in1[part].astype(F32)
        full_out1[side] = down_out[...].astype(BF16)
        full1.append(
            remote(full_out1.at[side], full_in1.at[side], f1_send.at[side], f1_recv.at[side], device(way, 0))
        )
        full1[-1].start()
    down_out[...] = ring_sum(3)
    for copy in full1:
        copy.wait_recv()
    down_out[...] += full_in1[0].astype(F32) + full_in1[1].astype(F32)
    outs.append(pltpu.make_async_copy(down_out, d_down, out_sem.at[2]))
    outs[-1].start()

    for copy in (*sent, *far, *full1, swap_parts, swap_acc):
        copy.wait_send()

    def drain(n, carry):
        for side, part in enumerate((lo, hi)):
            remote(far_out.at[n, part], half_in.at[n, part], a_send.at[n, side], h_recv.at[n, side], twin).wait_send()
            remote(full_out.at[n, side], full_in.at[n, side], f_send.at[n, side], f_recv.at[n, side], twin).wait_send()
        return carry

    lax.fori_loop(0, 4, drain, 0)
    for copy in outs:
        copy.wait()


def local(grad_out, gate_pre, up_pre, down_weight, new_logp, behav_logp, lengths, versions, token_lag):
    tokens, ff = gate_pre.shape
    rows = down_weight.shape[0]
    width = grad_out.shape[1]
    low = 40
    hbm = pl.BlockSpec(memory_space=pl.ANY)
    vmem = pl.BlockSpec(memory_space=pltpu.VMEM)
    smem = pl.BlockSpec(memory_space=pltpu.SMEM)
    dma = pltpu.SemaphoreType.DMA

    def line(values):
        return values.reshape(1, tokens)

    scratch = [
        pltpu.VMEM((16, rows, ff), BF16),
        pltpu.VMEM((7, tokens, width), BF16),
        pltpu.VMEM((tokens, width), BF16),
        pltpu.VMEM((2 * tokens, ff), BF16),
        pltpu.VMEM((tokens, ff), BF16),
        pltpu.VMEM((tokens, ff), BF16),
        pltpu.VMEM((tokens, ff), F32),
        pltpu.VMEM((tokens, ff), F32),
        pltpu.VMEM((16, 2 * tokens, 128), BF16),
        pltpu.VMEM((16, tokens, 128), BF16),
        pltpu.VMEM((2 * tokens, ff), F32),
        pltpu.VMEM((tokens, ff), F32),
        pltpu.VMEM((3, 16, tokens), F32),
        pltpu.VMEM((7, 16, tokens), F32),
        pltpu.VMEM((4, 3, rows, ff), F32),
        pltpu.VMEM((4, rows, ff), BF16),
        pltpu.VMEM((4, 2, rows, ff), BF16),
        pltpu.VMEM((4, rows, ff), BF16),
        pltpu.VMEM((4, 2, rows, ff), BF16),
        pltpu.VMEM((rows, ff), BF16),
        pltpu.VMEM((2, rows, ff), BF16),
        pltpu.VMEM((rows, ff), BF16),
        pltpu.VMEM((2, rows, ff), BF16),
        pltpu.VMEM((tokens, ff), BF16),
        pltpu.VMEM((tokens, ff), BF16),
        pltpu.VMEM((rows, ff), F32),
        dma((4,)), dma((3,)), dma((7,)), dma((7,)), dma((7,)), dma((7,)), dma((20,)), dma((20,)), dma((3,)), dma((3,)),
        dma((4, 2)), dma((4, 2)), dma((4, 2)), dma((4, 2)), dma((2,)), dma((2,)), dma((2,)), dma((2,)),
    ]
    return pl.pallas_call(
        functools.partial(kernel, rows, low),
        out_shape=(
            jax.ShapeDtypeStruct((tokens, ff), BF16),
            jax.ShapeDtypeStruct((tokens, ff), BF16),
            jax.ShapeDtypeStruct((rows, ff), F32),
        ),
        in_specs=[hbm, hbm, hbm, hbm, vmem, vmem, vmem, smem, smem],
        out_specs=(hbm, hbm, hbm),
        scratch_shapes=scratch,
        compiler_params=pltpu.CompilerParams(
            collective_id=0, has_side_effects=True, vmem_limit_bytes=60 * 1024 * 1024
        ),
    )(
        down_weight, grad_out, gate_pre, up_pre, line(new_logp), line(behav_logp), line(token_lag), lengths, versions
    )


def solution(mesh):
    split = Mesh(mesh.devices.reshape(4, 4, 2, mesh.shape["mp"]), (*DP, "mp"))
    placed = (P(DP, "mp"), P(DP, "mp"), P(DP, "mp"), P(DP, "mp"), P(DP), P(DP), P(DP), P(DP), P(DP))
    return jax.shard_map(
        local,
        mesh=split,
        in_specs=placed,
        out_specs=(P(DP, "mp"), P(DP, "mp"), P(DP, "mp")),
        check_vma=False,
    )
```

```python
import functools
import math

import jax
import jax.numpy as jnp
from jax import lax
from jax.experimental import pallas as pl
from jax.experimental.pallas import tpu as pltpu
from jax.sharding import Mesh
from jax.sharding import PartitionSpec as P

MAX_LAG = 5
DP = ("dp_0", "dp_1", "dp_2")
MESH = pl.DeviceIdType.MESH
F32, BF16 = jnp.float32, jnp.bfloat16
RATIO_CAP = 2.0
ROOT = math.sqrt(2.0 / math.pi)
CUBIC = 0.044715


def kernel(
    rows, low, weight, cotangent, gate, up, new_logp, old_logp, lag, length, version,
    d_gate, d_up, d_down,
    weights_all, cot_all, hidden, gate_v, up_v, act, up_slope, parts, others, acc, acc_in, hist_out, hist_in,
    new_v, old_v, lag_v,
    partial, far_out, full_out, half_in, full_in, far_out1, full_out1, half_in1, full_in1, gate_out, up_out, down_out,
    copy_sem, out_sem, hist_send, hist_recv, z_send, z_recv, ag_send, ag_recv, core_send, core_recv,
    a_send, f_send, h_recv, f_recv, a1_send, f1_send, h1_recv, f1_recv,
):
    y, x, c, z = (lax.axis_index(name) for name in (*DP, "mp"))
    tokens, units = hidden.shape[0] // 2, hidden.shape[1]
    lo, hi = pl.ds(0, low), pl.ds(low, rows - low)

    def at(i, j):
        return (
            lax.rem(y + 4 + i * c + j * (1 - c), 4),
            lax.rem(x + 4 + i * (1 - c) + j * c, 4),
        )

    def device(i, j):
        yy, xx = at(i, j)
        return (yy, xx, c, z)

    def block(i, j):
        yy, xx = at(i, j)
        return yy * 4 + xx

    twin = (y, x, 1 - c, z)
    z_peers = {d: (y, x, c, lax.rem(z + 8 + d, 8)) for d in (-2, 2, -1, 1)}
    x_peers = [(y, lax.rem(x + d, 4), c, z) for d in range(1, 4)]
    y_peers = [(lax.rem(y + d, 4), x, c, z) for d in range(1, 4)]
    peers = [twin, *z_peers.values(), *x_peers, *y_peers]

    def remote(src, dst, send, recv, to):
        return pltpu.make_async_remote_copy(
            src_ref=src, dst_ref=dst, send_sem=send, recv_sem=recv, device_id=to, device_id_type=MESH
        )

    barrier = pltpu.get_barrier_semaphore()
    for peer in peers:
        pl.semaphore_signal(barrier, inc=1, device_id=peer, device_id_type=MESH)

    own = block(0, 0)
    local = [
        pltpu.make_async_copy(gate, gate_v, copy_sem.at[0]),
        pltpu.make_async_copy(up, up_v, copy_sem.at[1]),
        pltpu.make_async_copy(cotangent, cot_all.at[0], copy_sem.at[2]),
        pltpu.make_async_copy(weight, weights_all.at[own], copy_sem.at[3]),
    ]
    small = [
        pltpu.make_async_copy(src, dst, copy_sem.at[4 + n])
        for n, (src, dst) in enumerate(((lag, lag_v), (new_logp, new_v), (old_logp, old_v)))
    ]
    for copy in (*small, *local):
        copy.start()
    for copy in small:
        copy.wait()

    bins = lax.broadcasted_iota(jnp.int32, (16, tokens), 0)
    position = lax.broadcasted_iota(jnp.int32, (1, tokens), 1)
    live = position < length[0]
    token_version = lag_v[...] + version[0]
    match = jnp.where((token_version == bins) & live, 1.0, 0.0)
    counts = jnp.broadcast_to(jnp.sum(match, axis=1, keepdims=True), (16, tokens))
    hist_out[0] = counts

    pl.semaphore_wait(barrier, len(peers))

    sent = []

    def go(copy):
        copy.start()
        sent.append(copy)

    for d in range(3):
        go(remote(hist_out.at[0], hist_in.at[d], hist_send.at[d], hist_recv.at[d], x_peers[d]))

    fulls = {(-1, 0): 0, (1, 0): 1, (0, -1): 2, (0, 1): 3, (-1, -1): 4, (-1, 1): 5, (1, -1): 6, (1, 1): 7, (2, -1): 8, (2, 1): 9}
    halves = {(2, 0): 10, (0, 2): 12, (-1, 2): 14, (1, 2): 16, (2, 2): 18}
    steps = {0: (1, 0), 1: (-1, 0), 2: (0, 1), 3: (0, -1)}

    def forward(i, j, way, half=None, src=None):
        di, dj = steps[way]
        slot = weights_all.at[block(i, j)]
        ni, nj = i - di, j - dj
        if half is None:
            sem = fulls[(ni, nj)]
            part = slot
        else:
            ni, nj = (2 if ni in (-2, 2) else ni), (2 if nj in (-2, 2) else nj)
            sem = halves[(ni, nj)] + half
            part = slot.at[lo if half == 0 else hi]
        go(remote(part if src is None else src, part, ag_send.at[len(used)], ag_recv.at[sem], device(di, dj)))
        used.append(sem)

    used = []

    def landed(i, j, half=None):
        slot = weights_all.at[block(i, j)]
        if half is None:
            sem, part = fulls[(i, j)], slot
        else:
            sem, part = halves[(i, j)] + half, slot.at[lo if half == 0 else hi]
        remote(part, part, ag_send.at[0], ag_recv.at[sem], twin).wait_recv()

    for way in range(4):
        forward(0, 0, way, src=weight)
    width = cotangent.shape[0]
    front, back = pl.ds(0, width // 2), pl.ds(width // 2, width // 2)

    def z_wait(d, half=None):
        part = cot_all.at[d] if half is None else cot_all.at[d, (front, back)[half]]
        sem = d - 1 if half is None else (3, 7)[half]
        remote(part, part, z_send.at[0], z_recv.at[sem], twin).wait_recv()

    for n, (d, slot) in enumerate(((2, 2), (-2, 6), (1, 1), (-1, 7))):
        go(remote(cotangent, cot_all.at[slot], z_send.at[n], z_recv.at[slot - 1], z_peers[d]))

    local[0].wait()
    local[1].wait()

    def elementwise(start, size):
        here = pl.ds(start, size)
        v = gate_v[here].astype(F32)
        u = up_v[here].astype(F32)
        square = v * v
        t = jnp.tanh(ROOT * (v + CUBIC * (square * v)))
        half = 0.5 * (1.0 + t)
        a = v * half
        slope = half + (0.5 * v) * (1.0 - t * t) * (ROOT * (1.0 + (3.0 * CUBIC) * square))
        act[here] = a
        up_slope[here] = u * slope
        hidden[pl.ds(0, tokens), here] = (a * u).T.astype(BF16)

    def over_units(body):
        def step(n, carry):
            body(pl.multiple_of(n * 128, 128), 128)
            return carry

        lax.fori_loop(0, units // 128, step, 0)
        if units % 128:
            body(units // 128 * 128, units % 128)

    over_units(elementwise)
    mine, theirs = pl.ds(0, tokens), pl.ds(tokens, tokens)
    swap_hidden = remote(hidden.at[mine], hidden.at[theirs], core_send.at[0], core_recv.at[0], twin)
    swap_hidden.start()

    def received(n):
        remote(hist_in.at[n], hist_in.at[n], hist_send.at[n], hist_recv.at[n], twin).wait_recv()
        return hist_in[n]

    counts = counts + received(0) + received(1) + received(2)
    hist_out[1] = counts
    for d in range(3):
        go(remote(hist_out.at[1], hist_in.at[3 + d], hist_send.at[3 + d], hist_recv.at[3 + d], y_peers[d]))

    z_wait(2)
    go(remote(cot_all.at[2], cot_all.at[3], z_send.at[4], z_recv.at[2], z_peers[1]))
    go(remote(cot_all.at[2, front], cot_all.at[4, front], z_send.at[5], z_recv.at[3], z_peers[2]))
    z_wait(6)
    go(remote(cot_all.at[6], cot_all.at[5], z_send.at[6], z_recv.at[4], z_peers[-1]))
    go(remote(cot_all.at[6, back], cot_all.at[4, back], z_send.at[7], z_recv.at[7], z_peers[-2]))

    for i in (-1, 1):
        landed(i, 0)
        forward(i, 0, 0 if i == -1 else 1, half=0 if i == -1 else 1)
        forward(i, 0, 2)
        forward(i, 0, 3)

    counts = counts + received(3) + received(4) + received(5)
    hist_out[2] = counts
    go(remote(hist_out.at[2], hist_in.at[6], hist_send.at[6], hist_recv.at[6], twin))

    def pass_on(i):
        landed(i, -1)
        forward(i, -1, 2, half=0)
        landed(i, 1)
        forward(i, 1, 3, half=1)

    counts = counts + received(6)
    current = jnp.max(jnp.where(counts > 0, bins, -1), axis=0, keepdims=True)
    oldest = current - MAX_LAG
    valid_count = jnp.sum(jnp.where(bins >= oldest, counts, 0.0), axis=0, keepdims=True)
    valid = live & (token_version >= oldest)
    ratio = jnp.minimum(jnp.exp(new_v[...] - old_v[...]), RATIO_CAP)
    token_weight = jnp.where(valid, ratio, 0.0) * (32.0 / valid_count)

    tall = parts.shape[1]
    line = lax.broadcasted_iota(jnp.int32, (4 * tall, width), 0)
    source = lax.broadcasted_iota(jnp.int32, (4 * tall, width), 1)
    group = (line >= tall).astype(jnp.int32) + (line >= 2 * tall).astype(jnp.int32) + (line >= 3 * tall).astype(jnp.int32)
    row = line - tall * group
    parity = jnp.where(group < 2, c, 1 - c)
    wanted = rows * (2 * (group & 1) + parity) + row
    select = jnp.where((source == wanted) & (row < rows), 1.0, 0.0).astype(BF16)

    def place(d):
        owner = lax.rem(z + 8 - d, 8)
        scaled = (token_weight * cot_all[d].astype(F32)).astype(BF16)
        picked = jnp.dot(select, scaled, preferred_element_type=F32).astype(BF16)
        for k in range(2):
            parts[2 * owner + k, :, pl.ds(0, tokens)] = picked[k * tall : (k + 1) * tall]
            others[2 * owner + k] = picked[(k + 2) * tall : (k + 3) * tall]

    local[2].wait()
    place(0)
    pass_on(0)
    for d in (2, 6, 1, 7):
        if d in (1, 7):
            z_wait(d)
        place(d)
    landed(2, 0, 0)
    landed(2, 0, 1)
    forward(2, 0, 2)
    forward(2, 0, 3)
    pass_on(-1)
    for d in (3, 5):
        z_wait(d)
        place(d)
    z_wait(4, 0)
    z_wait(4, 1)
    place(4)
    swap_parts = remote(others, parts.at[:, :, theirs], core_send.at[1], core_recv.at[1], twin)
    swap_parts.start()
    pass_on(1)
    swap_hidden.wait()
    swap_parts.wait_recv()

    def product(p):
        return jnp.dot(parts[p], hidden[...], preferred_element_type=F32)[:rows]

    def offset(n):
        return jnp.where(n < 2, n + 2, 3 - n)

    def start_far(n, carry):
        far_out[n] = product(block(offset(n), 2)).astype(BF16)
        remote(far_out.at[n, lo], half_in.at[n, lo], a_send.at[n, 0], h_recv.at[n, 0], device(0, 1)).start()
        remote(far_out.at[n, hi], half_in.at[n, hi], a_send.at[n, 1], h_recv.at[n, 1], device(0, -1)).start()
        return carry

    lax.fori_loop(0, 4, start_far, 0)

    def pass_full(n, carry):
        for side, (part, way) in enumerate(((lo, 1), (hi, -1))):
            partial[n, side] = product(block(offset(n), (1, 3)[side]))
            remote(half_in.at[n, part], half_in.at[n, part], a_send.at[n, side], h_recv.at[n, side], twin).wait_recv()
            first = partial[n, side, lo]
            second = partial[n, side, hi]
            arrived = half_in[n, part].astype(F32)
            if side == 0:
                first = first + arrived
            else:
                second = second + arrived
            full_out[n, side, lo] = first.astype(BF16)
            full_out[n, side, hi] = second.astype(BF16)
            remote(full_out.at[n, side], full_in.at[n, side], f_send.at[n, side], f_recv.at[n, side], device(0, way)).start()
        return carry

    lax.fori_loop(0, 4, pass_full, 0)
    pass_on(2)

    def rest(n, carry):
        partial[n, 2] = product(block(offset(n), 0))
        return carry

    lax.fori_loop(0, 4, rest, 0)

    for i in (0, -1, 1, 2):
        landed(i, 2, 0)
        landed(i, 2, 1)
    local[3].wait()
    acc[...] = jnp.zeros_like(acc)

    def accumulate(p, carry):
        acc[...] += lax.dot_general(
            parts[p, pl.ds(0, rows)], weights_all[p], (((0,), (0,)), ((), ())), preferred_element_type=F32
        )
        return carry

    lax.fori_loop(0, 16, accumulate, 0)
    swap_acc = remote(acc.at[theirs], acc_in, core_send.at[2], core_recv.at[2], twin)
    swap_acc.start()

    def finish(start, size):
        here = pl.ds(start, size)
        total = (acc[mine, here] + acc_in[:, here]).T
        up_out[here] = (total * act[here]).astype(BF16)
        gate_out[here] = (total * up_slope[here]).astype(BF16)

    outs = []

    def write_tokens():
        swap_acc.wait_recv()
        over_units(finish)
        for n, (src, dst) in enumerate(((gate_out, d_gate), (up_out, d_up))):
            outs.append(pltpu.make_async_copy(src, dst, out_sem.at[n]))
            outs[-1].start()

    def ring_sum(n):
        for side in range(2):
            remote(full_in.at[n, side], full_in.at[n, side], f_send.at[n, side], f_recv.at[n, side], twin).wait_recv()
        return partial[n, 2] + full_in[n, 0].astype(F32) + full_in[n, 1].astype(F32)

    far_out1[...] = ring_sum(0).astype(BF16)
    far = [
        remote(far_out1.at[part], half_in1.at[part], a1_send.at[side], h1_recv.at[side], device(way, 0))
        for side, (part, way) in enumerate(((lo, 1), (hi, -1)))
    ]
    for copy in far:
        copy.start()
    write_tokens()
    full1 = []
    for n, side in ((1, 1), (2, 0)):
        down_out[...] = ring_sum(n)
        part, way = ((lo, 1), (hi, -1))[side]
        far[side].wait_recv()
        down_out[part] += half_in1[part].astype(F32)
        full_out1[side] = down_out[...].astype(BF16)
        full1.append(
            remote(full_out1.at[side], full_in1.at[side], f1_send.at[side], f1_recv.at[side], device(way, 0))
        )
        full1[-1].start()
    down_out[...] = ring_sum(3)
    for copy in full1:
        copy.wait_recv()
    down_out[...] += full_in1[0].astype(F32) + full_in1[1].astype(F32)
    outs.append(pltpu.make_async_copy(down_out, d_down, out_sem.at[2]))
    outs[-1].start()

    for copy in (*sent, *far, *full1, swap_parts, swap_acc):
        copy.wait_send()

    def drain(n, carry):
        for side, part in enumerate((lo, hi)):
            remote(far_out.at[n, part], half_in.at[n, part], a_send.at[n, side], h_recv.at[n, side], twin).wait_send()
            remote(full_out.at[n, side], full_in.at[n, side], f_send.at[n, side], f_recv.at[n, side], twin).wait_send()
        return carry

    lax.fori_loop(0, 4, drain, 0)
    for copy in outs:
        copy.wait()


def local(grad_out, gate_pre, up_pre, down_weight, new_logp, behav_logp, lengths, versions, token_lag):
    tokens, ff = gate_pre.shape
    rows = down_weight.shape[0]
    width = grad_out.shape[1]
    low, tall = 40, 96
    hbm = pl.BlockSpec(memory_space=pl.ANY)
    smem = pl.BlockSpec(memory_space=pltpu.SMEM)
    dma = pltpu.SemaphoreType.DMA

    def line(values):
        return values.reshape(1, tokens)

    scratch = [
        pltpu.VMEM((16, rows, ff), BF16),
        pltpu.VMEM((8, width, tokens), BF16),
        pltpu.VMEM((2 * tokens, ff), BF16),
        pltpu.VMEM((ff, tokens), BF16),
        pltpu.VMEM((ff, tokens), BF16),
        pltpu.VMEM((ff, tokens), F32),
        pltpu.VMEM((ff, tokens), F32),
        pltpu.VMEM((16, tall, 2 * tokens), BF16),
        pltpu.VMEM((16, tall, tokens), BF16),
        pltpu.VMEM((2 * tokens, ff), F32),
        pltpu.VMEM((tokens, ff), F32),
        pltpu.VMEM((3, 16, tokens), F32),
        pltpu.VMEM((7, 16, tokens), F32),
        pltpu.VMEM((1, tokens), F32),
        pltpu.VMEM((1, tokens), F32),
        pltpu.VMEM((1, tokens), jnp.int32),
        pltpu.VMEM((4, 3, rows, ff), F32),
        pltpu.VMEM((4, rows, ff), BF16),
        pltpu.VMEM((4, 2, rows, ff), BF16),
        pltpu.VMEM((4, rows, ff), BF16),
        pltpu.VMEM((4, 2, rows, ff), BF16),
        pltpu.VMEM((rows, ff), BF16),
        pltpu.VMEM((2, rows, ff), BF16),
        pltpu.VMEM((rows, ff), BF16),
        pltpu.VMEM((2, rows, ff), BF16),
        pltpu.VMEM((ff, tokens), BF16),
        pltpu.VMEM((ff, tokens), BF16),
        pltpu.VMEM((rows, ff), F32),
        dma((7,)), dma((3,)), dma((7,)), dma((7,)), dma((8,)), dma((8,)), dma((20,)), dma((20,)), dma((3,)), dma((3,)),
        dma((4, 2)), dma((4, 2)), dma((4, 2)), dma((4, 2)), dma((2,)), dma((2,)), dma((2,)), dma((2,)),
    ]
    d_gate, d_up, d_down = pl.pallas_call(
        functools.partial(kernel, rows, low),
        out_shape=(
            jax.ShapeDtypeStruct((ff, tokens), BF16),
            jax.ShapeDtypeStruct((ff, tokens), BF16),
            jax.ShapeDtypeStruct((rows, ff), F32),
        ),
        in_specs=[hbm, hbm, hbm, hbm, hbm, hbm, hbm, smem, smem],
        out_specs=(hbm, hbm, hbm),
        scratch_shapes=scratch,
        compiler_params=pltpu.CompilerParams(
            collective_id=0, has_side_effects=True, vmem_limit_bytes=60 * 1024 * 1024
        ),
    )(
        down_weight, grad_out.T, gate_pre.T, up_pre.T, line(new_logp), line(behav_logp), line(token_lag), lengths, versions
    )
    return d_gate.T, d_up.T, d_down


def solution(mesh):
    split = Mesh(mesh.devices.reshape(4, 4, 2, mesh.shape["mp"]), (*DP, "mp"))
    placed = (P(DP, "mp"), P(DP, "mp"), P(DP, "mp"), P(DP, "mp"), P(DP), P(DP), P(DP), P(DP), P(DP))
    return jax.shard_map(
        local,
        mesh=split,
        in_specs=placed,
        out_specs=(P(DP, "mp"), P(DP, "mp"), P(DP, "mp")),
        check_vma=False,
    )
```

```python
import functools
import math

import jax
import jax.numpy as jnp
from jax import lax
from jax.experimental import pallas as pl
from jax.experimental.pallas import tpu as pltpu
from jax.sharding import Mesh
from jax.sharding import PartitionSpec as P

MAX_LAG = 5
DP = ("dp_0", "dp_1", "dp_2")
MESH = pl.DeviceIdType.MESH
F32, BF16 = jnp.float32, jnp.bfloat16
RATIO_CAP = 2.0
ROOT = math.sqrt(2.0 / math.pi)
CUBIC = 0.044715


def kernel(
    rows, low, weight, cotangent, gate, up, new_logp, old_logp, lag, length, version,
    gate_out, up_out, down_out,
    weights_all, cot_all, hidden, gate_v, up_v, act, up_slope, parts, others, acc, acc_in, hist_out, hist_in,
    new_v, old_v, lag_v,
    partial, far_out, full_out, half_in, full_in, far_out1, full_out1, half_in1, full_in1,
    copy_sem, hist_send, hist_recv, z_send, z_recv, ag_send, ag_recv, core_send, core_recv,
    a_send, f_send, h_recv, f_recv, a1_send, f1_send, h1_recv, f1_recv,
):
    y, x, c, z = (lax.axis_index(name) for name in (*DP, "mp"))
    tokens, units = hidden.shape[0] // 2, hidden.shape[1]
    lo, hi = pl.ds(0, low), pl.ds(low, rows - low)

    def at(i, j):
        return (
            lax.rem(y + 4 + i * c + j * (1 - c), 4),
            lax.rem(x + 4 + i * (1 - c) + j * c, 4),
        )

    def device(i, j):
        yy, xx = at(i, j)
        return (yy, xx, c, z)

    def block(i, j):
        yy, xx = at(i, j)
        return yy * 4 + xx

    twin = (y, x, 1 - c, z)
    z_peers = {d: (y, x, c, lax.rem(z + 8 + d, 8)) for d in (-2, 2, -1, 1)}
    x_peers = [(y, lax.rem(x + d, 4), c, z) for d in range(1, 4)]
    y_peers = [(lax.rem(y + d, 4), x, c, z) for d in range(1, 4)]
    peers = [twin, *z_peers.values(), *x_peers, *y_peers]

    def remote(src, dst, send, recv, to):
        return pltpu.make_async_remote_copy(
            src_ref=src, dst_ref=dst, send_sem=send, recv_sem=recv, device_id=to, device_id_type=MESH
        )

    barrier = pltpu.get_barrier_semaphore()
    for peer in peers:
        pl.semaphore_signal(barrier, inc=1, device_id=peer, device_id_type=MESH)

    own = block(0, 0)
    local = [
        pltpu.make_async_copy(gate, gate_v, copy_sem.at[0]),
        pltpu.make_async_copy(up, up_v, copy_sem.at[1]),
        pltpu.make_async_copy(cotangent, cot_all.at[0], copy_sem.at[2]),
        pltpu.make_async_copy(weight, weights_all.at[own], copy_sem.at[3]),
    ]
    small = [
        pltpu.make_async_copy(src, dst, copy_sem.at[4 + n])
        for n, (src, dst) in enumerate(((lag, lag_v), (new_logp, new_v), (old_logp, old_v)))
    ]
    for copy in (*small, *local):
        copy.start()
    for copy in small:
        copy.wait()

    bins = lax.broadcasted_iota(jnp.int32, (16, tokens), 0)
    position = lax.broadcasted_iota(jnp.int32, (1, tokens), 1)
    live = position < length[0]
    token_version = lag_v[...] + version[0]
    match = jnp.where((token_version == bins) & live, 1.0, 0.0)
    counts = jnp.broadcast_to(jnp.sum(match, axis=1, keepdims=True), (16, tokens))
    hist_out[0] = counts

    local[0].wait()
    local[1].wait()

    def elementwise(start, size):
        here = pl.ds(start, size)
        v = gate_v[here].astype(F32)
        u = up_v[here].astype(F32)
        square = v * v
        t = jnp.tanh(ROOT * (v + CUBIC * (square * v)))
        half = 0.5 * (1.0 + t)
        a = v * half
        slope = half + (0.5 * v) * (1.0 - t * t) * (ROOT * (1.0 + (3.0 * CUBIC) * square))
        act[here] = a
        up_slope[here] = u * slope
        hidden[pl.ds(0, tokens), here] = (a * u).T.astype(BF16)

    def over_units(body, first, last):
        def step(n, carry):
            body(pl.multiple_of(n * 128, 128), 128)
            return carry

        lax.fori_loop(first, min(last, units // 128), step, 0)
        if last > units // 128 and units % 128:
            body(units // 128 * 128, units % 128)

    chunks = pl.cdiv(units, 128)
    early = 4
    over_units(elementwise, 0, early)
    pl.semaphore_wait(barrier, len(peers))

    sent = []

    def go(copy):
        copy.start()
        sent.append(copy)

    for d in range(3):
        go(remote(hist_out.at[0], hist_in.at[d], hist_send.at[d], hist_recv.at[d], x_peers[d]))

    fulls = {(-1, 0): 0, (1, 0): 1, (0, -1): 2, (0, 1): 3, (-1, -1): 4, (-1, 1): 5, (1, -1): 6, (1, 1): 7, (2, -1): 8, (2, 1): 9}
    halves = {(2, 0): 10, (0, 2): 12, (-1, 2): 14, (1, 2): 16, (2, 2): 18}
    steps = {0: (1, 0), 1: (-1, 0), 2: (0, 1), 3: (0, -1)}

    def forward(i, j, way, half=None, src=None):
        di, dj = steps[way]
        slot = weights_all.at[block(i, j)]
        ni, nj = i - di, j - dj
        if half is None:
            sem = fulls[(ni, nj)]
            part = slot
        else:
            ni, nj = (2 if ni in (-2, 2) else ni), (2 if nj in (-2, 2) else nj)
            sem = halves[(ni, nj)] + half
            part = slot.at[lo if half == 0 else hi]
        go(remote(part if src is None else src, part, ag_send.at[len(used)], ag_recv.at[sem], device(di, dj)))
        used.append(sem)

    used = []

    def landed(i, j, half=None):
        slot = weights_all.at[block(i, j)]
        if half is None:
            sem, part = fulls[(i, j)], slot
        else:
            sem, part = halves[(i, j)] + half, slot.at[lo if half == 0 else hi]
        remote(part, part, ag_send.at[0], ag_recv.at[sem], twin).wait_recv()

    for way in range(2):
        forward(0, 0, way, src=weight)
    width = cotangent.shape[0]
    front, back = pl.ds(0, width // 2), pl.ds(width // 2, width // 2)

    def z_wait(d, half=None):
        part = cot_all.at[d] if half is None else cot_all.at[d, (front, back)[half]]
        sem = d - 1 if half is None else (3, 7)[half]
        remote(part, part, z_send.at[0], z_recv.at[sem], twin).wait_recv()

    for n, (d, slot) in enumerate(((2, 2), (-2, 6), (1, 1), (-1, 7))):
        go(remote(cotangent, cot_all.at[slot], z_send.at[n], z_recv.at[slot - 1], z_peers[d]))

    over_units(elementwise, early, chunks)
    mine, theirs = pl.ds(0, tokens), pl.ds(tokens, tokens)
    swap_hidden = remote(hidden.at[mine], hidden.at[theirs], core_send.at[0], core_recv.at[0], twin)
    swap_hidden.start()

    def received(n):
        remote(hist_in.at[n], hist_in.at[n], hist_send.at[n], hist_recv.at[n], twin).wait_recv()
        return hist_in[n]

    counts = counts + received(0) + received(1) + received(2)
    hist_out[1] = counts
    for d in range(3):
        go(remote(hist_out.at[1], hist_in.at[3 + d], hist_send.at[3 + d], hist_recv.at[3 + d], y_peers[d]))

    for way in range(2, 4):
        forward(0, 0, way, src=weight)
    z_wait(2)
    go(remote(cot_all.at[2], cot_all.at[3], z_send.at[4], z_recv.at[2], z_peers[1]))
    go(remote(cot_all.at[2, front], cot_all.at[4, front], z_send.at[5], z_recv.at[3], z_peers[2]))
    z_wait(6)
    go(remote(cot_all.at[6], cot_all.at[5], z_send.at[6], z_recv.at[4], z_peers[-1]))
    go(remote(cot_all.at[6, back], cot_all.at[4, back], z_send.at[7], z_recv.at[7], z_peers[-2]))

    for i in (-1, 1):
        landed(i, 0)
        forward(i, 0, 0 if i == -1 else 1, half=0 if i == -1 else 1)
        forward(i, 0, 2)
        forward(i, 0, 3)

    counts = counts + received(3) + received(4) + received(5)
    hist_out[2] = counts
    go(remote(hist_out.at[2], hist_in.at[6], hist_send.at[6], hist_recv.at[6], twin))

    def pass_on(i):
        landed(i, -1)
        forward(i, -1, 2, half=0)
        landed(i, 1)
        forward(i, 1, 3, half=1)

    counts = counts + received(6)
    current = jnp.max(jnp.where(counts > 0, bins, -1), axis=0, keepdims=True)
    oldest = current - MAX_LAG
    valid_count = jnp.sum(jnp.where(bins >= oldest, counts, 0.0), axis=0, keepdims=True)
    valid = live & (token_version >= oldest)
    ratio = jnp.minimum(jnp.exp(new_v[...] - old_v[...]), RATIO_CAP)
    token_weight = jnp.where(valid, ratio, 0.0) * (32.0 / valid_count)

    tall = parts.shape[1]
    line = lax.broadcasted_iota(jnp.int32, (4 * tall, width), 0)
    source = lax.broadcasted_iota(jnp.int32, (4 * tall, width), 1)
    group = (line >= tall).astype(jnp.int32) + (line >= 2 * tall).astype(jnp.int32) + (line >= 3 * tall).astype(jnp.int32)
    row = line - tall * group
    parity = jnp.where(group < 2, c, 1 - c)
    wanted = rows * (2 * (group & 1) + parity) + row
    select = jnp.where((source == wanted) & (row < rows), 1.0, 0.0).astype(BF16)

    def place(d):
        owner = lax.rem(z + 8 - d, 8)
        scaled = (token_weight * cot_all[d].astype(F32)).astype(BF16)
        picked = jnp.dot(select, scaled, preferred_element_type=F32).astype(BF16)
        for k in range(2):
            parts[2 * owner + k, :, pl.ds(0, tokens)] = picked[k * tall : (k + 1) * tall]
            others[2 * owner + k] = picked[(k + 2) * tall : (k + 3) * tall]

    local[2].wait()
    place(0)
    place(2)
    place(6)
    pass_on(0)
    for d in (1, 7):
        z_wait(d)
        place(d)
    landed(2, 0, 0)
    landed(2, 0, 1)
    forward(2, 0, 2)
    forward(2, 0, 3)
    for d in (3, 5):
        z_wait(d)
        place(d)
    z_wait(4, 0)
    z_wait(4, 1)
    place(4)
    swap_parts = remote(others, parts.at[:, :, theirs], core_send.at[1], core_recv.at[1], twin)
    swap_parts.start()
    pass_on(-1)
    pass_on(1)
    swap_hidden.wait()
    swap_parts.wait_recv()

    def product(p):
        return jnp.dot(parts[p], hidden[...], preferred_element_type=F32)[:rows]

    def offset(n):
        return jnp.where(n < 2, n + 2, 3 - n)

    def start_far(n, carry):
        far_out[n] = product(block(offset(n), 2)).astype(BF16)
        remote(far_out.at[n, lo], half_in.at[n, lo], a_send.at[n, 0], h_recv.at[n, 0], device(0, 1)).start()
        remote(far_out.at[n, hi], half_in.at[n, hi], a_send.at[n, 1], h_recv.at[n, 1], device(0, -1)).start()
        return carry

    lax.fori_loop(0, 4, start_far, 0)

    def pass_full(n, carry):
        for side, (part, way) in enumerate(((lo, 1), (hi, -1))):
            partial[n, side] = product(block(offset(n), (1, 3)[side]))
            remote(half_in.at[n, part], half_in.at[n, part], a_send.at[n, side], h_recv.at[n, side], twin).wait_recv()
            first = partial[n, side, lo]
            second = partial[n, side, hi]
            arrived = half_in[n, part].astype(F32)
            if side == 0:
                first = first + arrived
            else:
                second = second + arrived
            full_out[n, side, lo] = first.astype(BF16)
            full_out[n, side, hi] = second.astype(BF16)
            remote(full_out.at[n, side], full_in.at[n, side], f_send.at[n, side], f_recv.at[n, side], device(0, way)).start()
        return carry

    def rest(n, carry):
        partial[n, 2] = product(block(offset(n), 0))
        return carry

    def accumulate(group, first=False):
        total = None if first else acc[...]
        for i, j in group:
            p = block(i, j)
            term = lax.dot_general(
                parts[p, pl.ds(0, rows)], weights_all[p], (((0,), (0,)), ((), ())), preferred_element_type=F32
            )
            total = term if total is None else total + term
        acc[...] = total

    local[3].wait()
    accumulate(((0, 0), (-1, 0), (1, 0), (2, 0)), first=True)
    lax.fori_loop(0, 4, pass_full, 0)
    pass_on(2)
    accumulate(((0, -1), (0, 1), (-1, -1), (-1, 1)))
    lax.fori_loop(0, 4, rest, 0)
    def finish(start, size):
        here = pl.ds(start, size)
        total = (acc[mine, here] + acc_in[:, here]).T
        up_out[here] = (total * act[here]).astype(BF16)
        gate_out[here] = (total * up_slope[here]).astype(BF16)

    def write_tokens():
        swap_acc.wait_recv()
        over_units(finish, 0, chunks)

    def ring_sum(n):
        for side in range(2):
            remote(full_in.at[n, side], full_in.at[n, side], f_send.at[n, side], f_recv.at[n, side], twin).wait_recv()
        return partial[n, 2] + full_in[n, 0].astype(F32) + full_in[n, 1].astype(F32)

    far_out1[...] = ring_sum(0).astype(BF16)
    far = [
        remote(far_out1.at[part], half_in1.at[part], a1_send.at[side], h1_recv.at[side], device(way, 0))
        for side, (part, way) in enumerate(((lo, 1), (hi, -1)))
    ]
    for copy in far:
        copy.start()
    accumulate(((1, -1), (1, 1), (2, -1), (2, 1)))
    full1 = []
    for n, side in ((1, 1), (2, 0)):
        down_out[...] = ring_sum(n)
        part, way = ((lo, 1), (hi, -1))[side]
        far[side].wait_recv()
        down_out[part] += half_in1[part].astype(F32)
        full_out1[side] = down_out[...].astype(BF16)
        full1.append(
            remote(full_out1.at[side], full_in1.at[side], f1_send.at[side], f1_recv.at[side], device(way, 0))
        )
        full1[-1].start()
    last = (0, -1, 1, 2)
    for i in last:
        landed(i, 2, 0)
        landed(i, 2, 1)
    accumulate([(i, 2) for i in last])
    swap_acc = remote(acc.at[theirs], acc_in, core_send.at[2], core_recv.at[2], twin)
    swap_acc.start()
    write_tokens()
    down_out[...] = ring_sum(3)
    for copy in full1:
        copy.wait_recv()
    down_out[...] += full_in1[0].astype(F32) + full_in1[1].astype(F32)

    for copy in (*sent, *far, *full1, swap_parts, swap_acc):
        copy.wait_send()

    def drain(n, carry):
        for side, part in enumerate((lo, hi)):
            remote(far_out.at[n, part], half_in.at[n, part], a_send.at[n, side], h_recv.at[n, side], twin).wait_send()
            remote(full_out.at[n, side], full_in.at[n, side], f_send.at[n, side], f_recv.at[n, side], twin).wait_send()
        return carry

    lax.fori_loop(0, 4, drain, 0)


def write_out(*refs):
    sem = refs[-1]
    copies = [pltpu.make_async_copy(refs[n], refs[3 + n], sem.at[n]) for n in range(3)]
    for copy in copies:
        copy.start()
    for copy in copies:
        copy.wait()


def local(grad_out, gate_pre, up_pre, down_weight, new_logp, behav_logp, lengths, versions, token_lag):
    tokens, ff = gate_pre.shape
    rows = down_weight.shape[0]
    width = grad_out.shape[1]
    low, tall = 40, 96
    hbm = pl.BlockSpec(memory_space=pl.ANY)
    smem = pl.BlockSpec(memory_space=pltpu.SMEM)
    dma = pltpu.SemaphoreType.DMA

    def line(values):
        return values.reshape(1, tokens)

    scratch = [
        pltpu.VMEM((16, rows, ff), BF16),
        pltpu.VMEM((8, width, tokens), BF16),
        pltpu.VMEM((2 * tokens, ff), BF16),
        pltpu.VMEM((ff, tokens), BF16),
        pltpu.VMEM((ff, tokens), BF16),
        pltpu.VMEM((ff, tokens), F32),
        pltpu.VMEM((ff, tokens), F32),
        pltpu.VMEM((16, tall, 2 * tokens), BF16),
        pltpu.VMEM((16, tall, tokens), BF16),
        pltpu.VMEM((2 * tokens, ff), F32),
        pltpu.VMEM((tokens, ff), F32),
        pltpu.VMEM((3, 16, tokens), F32),
        pltpu.VMEM((7, 16, tokens), F32),
        pltpu.VMEM((1, tokens), F32),
        pltpu.VMEM((1, tokens), F32),
        pltpu.VMEM((1, tokens), jnp.int32),
        pltpu.VMEM((4, 3, rows, ff), F32),
        pltpu.VMEM((4, rows, ff), BF16),
        pltpu.VMEM((4, 2, rows, ff), BF16),
        pltpu.VMEM((4, rows, ff), BF16),
        pltpu.VMEM((4, 2, rows, ff), BF16),
        pltpu.VMEM((rows, ff), BF16),
        pltpu.VMEM((2, rows, ff), BF16),
        pltpu.VMEM((rows, ff), BF16),
        pltpu.VMEM((2, rows, ff), BF16),
        dma((7,)), dma((7,)), dma((7,)), dma((8,)), dma((8,)), dma((20,)), dma((20,)), dma((3,)), dma((3,)),
        dma((4, 2)), dma((4, 2)), dma((4, 2)), dma((4, 2)), dma((2,)), dma((2,)), dma((2,)), dma((2,)),
    ]
    outs = (
        jax.ShapeDtypeStruct((ff, tokens), BF16),
        jax.ShapeDtypeStruct((ff, tokens), BF16),
        jax.ShapeDtypeStruct((rows, ff), F32),
    )
    values = pl.pallas_call(
        functools.partial(kernel, rows, low),
        out_shape=tuple(pltpu.VMEM(o.shape, o.dtype) for o in outs),
        in_specs=[hbm, hbm, hbm, hbm, hbm, hbm, hbm, smem, smem],
        out_specs=(pl.BlockSpec(memory_space=pltpu.VMEM),) * 3,
        scratch_shapes=scratch,
        compiler_params=pltpu.CompilerParams(
            collective_id=0, has_side_effects=True, vmem_limit_bytes=60 * 1024 * 1024
        ),
    )(
        down_weight, grad_out.T, gate_pre.T, up_pre.T, line(new_logp), line(behav_logp), line(token_lag), lengths, versions
    )
    d_gate, d_up, d_down = pl.pallas_call(
        write_out,
        out_shape=outs,
        in_specs=[pl.BlockSpec(memory_space=pltpu.VMEM)] * 3,
        out_specs=(hbm, hbm, hbm),
        scratch_shapes=[dma((3,))],
    )(*(pltpu.with_memory_space_constraint(v, pltpu.VMEM) for v in values))
    return d_gate.T, d_up.T, d_down


def solution(mesh):
    split = Mesh(mesh.devices.reshape(4, 4, 2, mesh.shape["mp"]), (*DP, "mp"))
    placed = (P(DP, "mp"), P(DP, "mp"), P(DP, "mp"), P(DP, "mp"), P(DP), P(DP), P(DP), P(DP), P(DP))
    return jax.shard_map(
        local,
        mesh=split,
        in_specs=placed,
        out_specs=(P(DP, "mp"), P(DP, "mp"), P(DP, "mp")),
        check_vma=False,
    )
```

```python
import functools
import math

import jax
import jax.numpy as jnp
from jax import lax
from jax.experimental import pallas as pl
from jax.experimental.pallas import tpu as pltpu
from jax.sharding import Mesh
from jax.sharding import PartitionSpec as P

MAX_LAG = 5
DP = ("dp_0", "dp_1", "dp_2")
MESH = pl.DeviceIdType.MESH
F32, BF16 = jnp.float32, jnp.bfloat16
RATIO_CAP = 2.0
ROOT = math.sqrt(2.0 / math.pi)
CUBIC = 0.044715


def kernel(
    rows, low, weight, cotangent, gate, up, new_logp, old_logp, lag, length, version,
    gate_out, up_out, down_out,
    weights_all, cot_all, hidden, gate_v, up_v, act, up_slope, pool, others, far, acc, acc_in, sum_out, sum_in, hist_out, hist_in,
    new_v, old_v, lag_v, partial, a_out, b_out, c_out, d_out, e_out, a_in, b_in, c_in, d_in, e_in,
    copy_sem, hist_send, hist_recv, z_send, z_recv, ag_send, ag_recv, core_send, core_recv, swap_send, swap_recv,
    cross_send, cross_recv, far_send, far_recv, rs_send, rs_recv,
):
    y, x, c, z = (lax.axis_index(name) for name in (*DP, "mp"))
    tokens, units = hidden.shape[0] // 4, hidden.shape[1]
    lo, hi = pl.ds(0, low), pl.ds(low, rows - low)
    side, column = x // 2, lax.rem(x, 2)

    def block(i, j):
        return lax.rem(y + 4 + j, 4) * 2 + lax.rem(column + i, 2)

    twin = (y, x, 1 - c, z)
    beside = (y, x + 1 - 2 * column, c, z)
    across = (y, 3 - x, c, z)
    ahead, behind = (lax.rem(y + 1, 4), x, c, z), (lax.rem(y + 3, 4), x, c, z)
    z_peers = {d: (y, x, c, lax.rem(z + 8 + d, 8)) for d in (-2, 2, -1, 1)}
    x_peers = [(y, lax.rem(x + d, 4), c, z) for d in range(1, 4)]
    y_peers = [(lax.rem(y + d, 4), x, c, z) for d in range(1, 4)]
    peers = [twin, *z_peers.values(), *x_peers, *y_peers]

    def remote(src, dst, send, recv, to):
        return pltpu.make_async_remote_copy(
            src_ref=src, dst_ref=dst, send_sem=send, recv_sem=recv, device_id=to, device_id_type=MESH
        )

    barrier = pltpu.get_barrier_semaphore()
    for peer in peers:
        pl.semaphore_signal(barrier, inc=1, device_id=peer, device_id_type=MESH)

    own = block(0, 0)
    local = [
        pltpu.make_async_copy(gate, gate_v, copy_sem.at[0]),
        pltpu.make_async_copy(up, up_v, copy_sem.at[1]),
        pltpu.make_async_copy(cotangent, cot_all.at[0], copy_sem.at[2]),
        pltpu.make_async_copy(weight, weights_all.at[own], copy_sem.at[3]),
    ]
    small = [
        pltpu.make_async_copy(src, dst, copy_sem.at[4 + n])
        for n, (src, dst) in enumerate(((lag, lag_v), (new_logp, new_v), (old_logp, old_v)))
    ]
    for copy in (*small, *local):
        copy.start()
    for copy in small:
        copy.wait()

    bins = lax.broadcasted_iota(jnp.int32, (16, tokens), 0)
    position = lax.broadcasted_iota(jnp.int32, (1, tokens), 1)
    live = position < length[0]
    token_version = lag_v[...] + version[0]
    match = jnp.where((token_version == bins) & live, 1.0, 0.0)
    counts = jnp.broadcast_to(jnp.sum(match, axis=1, keepdims=True), (16, tokens))
    hist_out[0] = counts

    local[0].wait()
    local[1].wait()

    def elementwise(start, size):
        here = pl.ds(start, size)
        v = gate_v[here].astype(F32)
        u = up_v[here].astype(F32)
        square = v * v
        t = jnp.tanh(ROOT * (v + CUBIC * (square * v)))
        half = 0.5 * (1.0 + t)
        a = v * half
        slope = half + (0.5 * v) * (1.0 - t * t) * (ROOT * (1.0 + (3.0 * CUBIC) * square))
        act[here] = a
        up_slope[here] = u * slope
        hidden[pl.ds(0, tokens), here] = (a * u).T.astype(BF16)

    def over_units(body, first, last):
        def step(n, carry):
            body(pl.multiple_of(n * 128, 128), 128)
            return carry

        lax.fori_loop(first, min(last, units // 128), step, 0)
        if last > units // 128 and units % 128:
            body(units // 128 * 128, units % 128)

    chunks = pl.cdiv(units, 128)
    early = 4
    over_units(elementwise, 0, early)
    pl.semaphore_wait(barrier, len(peers))

    sent = []

    def go(copy):
        copy.start()
        sent.append(copy)

    for d in range(3):
        go(remote(hist_out.at[0], hist_in.at[d], hist_send.at[d], hist_recv.at[d], x_peers[d]))

    slots = {(1, 0): 0, (0, -1): 1, (0, 1): 2, (1, -1): 3, (1, 1): 4, (0, 2): 5, (1, 2): 7}

    def spread(i, j, to, as_i, as_j, half=0, part=None, src=None):
        view = weights_all.at[block(i, j)]
        view = view if part is None else view.at[part]
        sem = slots[(as_i, as_j)] + half
        go(remote(view if src is None else src, view, ag_send.at[sem], ag_recv.at[sem], to))

    def landed(i, j, half=0, part=None):
        view = weights_all.at[block(i, j)]
        view = view if part is None else view.at[part]
        sem = slots[(i, j)] + half
        remote(view, view, ag_send.at[sem], ag_recv.at[sem], twin).wait_recv()

    width = cotangent.shape[0]
    front, back = pl.ds(0, width // 2), pl.ds(width // 2, width // 2)

    def z_wait(d, half=None):
        part = cot_all.at[d] if half is None else cot_all.at[d, (front, back)[half]]
        sem = d - 1 if half is None else (3, 7)[half]
        remote(part, part, z_send.at[0], z_recv.at[sem], twin).wait_recv()

    for n, (d, slot) in enumerate(((2, 2), (-2, 6), (1, 1), (-1, 7))):
        go(remote(cotangent, cot_all.at[slot], z_send.at[n], z_recv.at[slot - 1], z_peers[d]))
    spread(0, 0, beside, 1, 0, src=weight)
    spread(0, 0, ahead, 0, -1, src=weight)
    spread(0, 0, behind, 0, 1, src=weight)

    over_units(elementwise, early, chunks)
    quarter = [pl.ds(n * tokens, tokens) for n in range(4)]
    crossing = [
        remote(hidden.at[quarter[0]], hidden.at[quarter[2]], core_send.at[0], core_recv.at[0], across),
        remote(hidden.at[quarter[0]], hidden.at[quarter[1]], core_send.at[1], core_recv.at[1], twin),
        remote(hidden.at[quarter[2]], hidden.at[quarter[3]], core_send.at[2], core_recv.at[2], twin),
    ]
    crossing[0].start()
    crossing[1].start()

    def received(n):
        remote(hist_in.at[n], hist_in.at[n], hist_send.at[n], hist_recv.at[n], twin).wait_recv()
        return hist_in[n]

    counts = counts + received(0) + received(1) + received(2)
    hist_out[1] = counts
    for d in range(3):
        go(remote(hist_out.at[1], hist_in.at[3 + d], hist_send.at[3 + d], hist_recv.at[3 + d], y_peers[d]))

    z_wait(2)
    go(remote(cot_all.at[2], cot_all.at[3], z_send.at[4], z_recv.at[2], z_peers[1]))
    go(remote(cot_all.at[2, front], cot_all.at[4, front], z_send.at[5], z_recv.at[3], z_peers[2]))
    z_wait(6)
    go(remote(cot_all.at[6], cot_all.at[5], z_send.at[6], z_recv.at[4], z_peers[-1]))
    go(remote(cot_all.at[6, back], cot_all.at[4, back], z_send.at[7], z_recv.at[7], z_peers[-2]))

    counts = counts + received(3) + received(4) + received(5)
    hist_out[2] = counts
    go(remote(hist_out.at[2], hist_in.at[6], hist_send.at[6], hist_recv.at[6], twin))

    landed(1, 0)
    spread(1, 0, ahead, 1, -1)
    spread(1, 0, behind, 1, 1)
    landed(0, -1)
    spread(0, -1, ahead, 0, 2, 0, lo)
    landed(0, 1)
    spread(0, 1, behind, 0, 2, 1, hi)

    counts = counts + received(6)
    current = jnp.max(jnp.where(counts > 0, bins, -1), axis=0, keepdims=True)
    oldest = current - MAX_LAG
    valid_count = jnp.sum(jnp.where(bins >= oldest, counts, 0.0), axis=0, keepdims=True)
    valid = live & (token_version >= oldest)
    ratio = jnp.minimum(jnp.exp(new_v[...] - old_v[...]), RATIO_CAP)
    token_weight = jnp.where(valid, ratio, 0.0) * (32.0 / valid_count)

    tall = pool.shape[2]
    line = lax.broadcasted_iota(jnp.int32, (4 * tall, width), 0)
    source = lax.broadcasted_iota(jnp.int32, (4 * tall, width), 1)
    group = (line >= tall).astype(jnp.int32) + (line >= 2 * tall).astype(jnp.int32) + (line >= 3 * tall).astype(jnp.int32)
    row = line - tall * group
    parity = jnp.where(group < 2, c, 1 - c)
    wanted = rows * (2 * (group & 1) + parity) + row
    select = jnp.where((source == wanted) & (row < rows), 1.0, 0.0).astype(BF16)

    outgoing = lax.rem(z + side + 1, 2)

    def where(d):
        owner = lax.rem(z + 8 - d, 8)
        return lax.rem(owner, 2), owner // 2

    def swap(d):
        of, pair = where(d)
        pairs = pl.ds(pair * 2, 2)
        return remote(
            others.at[of, pairs], pool.at[of, pairs, :, pl.ds(tokens, tokens)], swap_send.at[d], swap_recv.at[d], twin
        )

    def place(d):
        of, pair = where(d)
        scaled = (token_weight * cot_all[d].astype(F32)).astype(BF16)
        picked = jnp.dot(select, scaled, preferred_element_type=F32)
        for k in range(2):
            pool[of, 2 * pair + k, :, pl.ds(0, tokens)] = picked[k * tall : (k + 1) * tall].astype(BF16)
            others[of, 2 * pair + k] = picked[(k + 2) * tall : (k + 3) * tall].astype(BF16)
        swap(d).start()

    def hand(pair):
        pairs = pl.ds(pair * 2, 2)
        return remote(pool.at[1 - side, pairs], far.at[pairs], far_send.at[pair], far_recv.at[pair], across)

    def export(d):
        swap(d).wait_recv()

        @pl.when(outgoing == d % 2)
        def _():
            hand(where(d)[1]).start()

    local[2].wait()
    for d in (0, 2, 6):
        place(d)
    for d in (1, 7):
        z_wait(d)
        place(d)
    for d in (0, 2, 6, 1, 7):
        export(d)
    landed(0, 2, 0, lo)
    landed(0, 2, 1, hi)
    spread(0, 2, beside, 1, 2)
    for d in (3, 5):
        z_wait(d)
        place(d)
    z_wait(4, 0)
    z_wait(4, 1)
    place(4)
    for d in (3, 5, 4):
        export(d)
    crossing[0].wait_recv()
    crossing[2].start()
    local[3].wait()
    landed(1, -1)
    landed(1, 1)
    landed(1, 2)

    near_rows, far_rows = pl.ds(0, 2 * tokens), pl.ds(2 * tokens, 2 * tokens)

    def accumulate(group, first):
        for source, here in ((pool.at[side], near_rows), (far, far_rows)):
            total = None if first else acc[here]
            for i, j in group:
                p = block(i, j)
                term = lax.dot_general(
                    source[p, pl.ds(0, rows)], weights_all[p], (((0,), (0,)), ((), ())), preferred_element_type=F32
                )
                total = term if total is None else total + term
            acc[here] = total

    crossing[1].wait_recv()
    for pair in range(4):
        hand(pair).wait_recv()
    crossing[2].wait_recv()

    targets = ((1, 2), (1, 1), (1, -1), (0, 2), (1, 0), (0, 1), (0, -1), (0, 0))

    def product(n, i, j):
        p = lax.rem(y + 4 + j, 4) * 2 + lax.rem(column + i, 2)
        near = jnp.dot(pool[side, p], hidden[near_rows], preferred_element_type=F32)
        partial[n] = (near + jnp.dot(far[p], hidden[far_rows], preferred_element_type=F32))[:rows]

    def shift(n):
        i = jnp.where((n < 3) | (n == 4), 1, 0)
        j = jnp.where((n == 0) | (n == 3), 2, jnp.where((n == 1) | (n == 5), 1, jnp.where((n == 2) | (n == 6), 3, 0)))
        return i, j

    def products(first, last):
        def step(n, carry):
            product(n, *shift(n))
            return carry

        lax.fori_loop(first, last, step, 0)

    sums = {
        "a": (a_out, a_in, 0, beside),
        "b0": (b_out.at[0], b_in.at[0], 1, ahead),
        "b1": (b_out.at[1], b_in.at[1], 2, behind),
        "c0": (c_out.at[lo], c_in.at[lo], 3, ahead),
        "c1": (c_out.at[hi], c_in.at[hi], 4, behind),
        "d": (d_out, d_in, 5, beside),
        "e0": (e_out.at[0], e_in.at[0], 6, ahead),
        "e1": (e_out.at[1], e_in.at[1], 7, behind),
    }
    sums = {key: remote(src, dst, rs_send.at[n], rs_recv.at[n], to) for key, (src, dst, n, to) in sums.items()}

    products(0, 3)
    a_out[...] = partial[0].astype(BF16)
    sums["a"].start()
    b_out[0] = partial[1].astype(BF16)
    sums["b0"].start()
    b_out[1] = partial[2].astype(BF16)
    sums["b1"].start()
    accumulate(((0, 0), (1, 0), (0, -1), (0, 1)), True)
    accumulate(((1, -1), (1, 1), (0, 2), (1, 2)), False)
    swaps = [
        remote(acc.at[quarter[2 * n + 1]], acc_in.at[n], cross_send.at[n], cross_recv.at[n], twin) for n in range(2)
    ]
    swaps[1].start()
    swaps[0].start()
    products(3, 8)
    sums["a"].wait_recv()
    c_out[...] = (partial[3] + a_in[...].astype(F32)).astype(BF16)
    sums["c0"].start()
    sums["c1"].start()
    swaps[1].wait_recv()
    sum_out[...] = (acc[quarter[2]] + acc_in[1]).astype(BF16)
    sum_cross = remote(sum_out, sum_in, cross_send.at[2], cross_recv.at[2], across)
    sum_cross.start()
    sums["b0"].wait_recv()
    sums["b1"].wait_recv()
    d_out[...] = (partial[4] + b_in[0].astype(F32) + b_in[1].astype(F32)).astype(BF16)
    sums["d"].start()
    sums["c0"].wait_recv()
    partial[5, lo] += c_in[lo].astype(F32)
    e_out[0] = partial[5].astype(BF16)
    sums["e0"].start()
    sums["c1"].wait_recv()
    partial[6, hi] += c_in[hi].astype(F32)
    e_out[1] = partial[6].astype(BF16)
    sums["e1"].start()

    def finish(start, size):
        here = pl.ds(start, size)
        total = (acc[quarter[0], here] + acc_in[0, :, here] + sum_in[:, here].astype(F32)).T
        up_out[here] = (total * act[here]).astype(BF16)
        gate_out[here] = (total * up_slope[here]).astype(BF16)

    swaps[0].wait_recv()
    sum_cross.wait_recv()
    over_units(finish, 0, chunks)
    sums["d"].wait_recv()
    down_out[...] = partial[7] + d_in[...].astype(F32)
    sums["e0"].wait_recv()
    sums["e1"].wait_recv()
    down_out[...] += e_in[0].astype(F32) + e_in[1].astype(F32)

    for copy in (*sent, *crossing, *swaps, sum_cross, *sums.values()):
        copy.wait_send()
    for d in range(8):
        swap(d).wait_send()
    for pair in range(4):
        hand(pair).wait_send()


def write_out(*refs):
    sem = refs[-1]
    copies = [pltpu.make_async_copy(refs[n], refs[3 + n], sem.at[n]) for n in range(3)]
    for copy in copies:
        copy.start()
    for copy in copies:
        copy.wait()


def local(grad_out, gate_pre, up_pre, down_weight, new_logp, behav_logp, lengths, versions, token_lag):
    tokens, ff = gate_pre.shape
    rows = down_weight.shape[0]
    width = grad_out.shape[1]
    low, tall = 40, 88
    hbm = pl.BlockSpec(memory_space=pl.ANY)
    smem = pl.BlockSpec(memory_space=pltpu.SMEM)
    dma = pltpu.SemaphoreType.DMA

    def line(values):
        return values.reshape(1, tokens)

    scratch = [
        pltpu.VMEM((8, rows, ff), BF16),
        pltpu.VMEM((8, width, tokens), BF16),
        pltpu.VMEM((4 * tokens, ff), BF16),
        pltpu.VMEM((ff, tokens), BF16),
        pltpu.VMEM((ff, tokens), BF16),
        pltpu.VMEM((ff, tokens), F32),
        pltpu.VMEM((ff, tokens), F32),
        pltpu.VMEM((2, 8, tall, 2 * tokens), BF16),
        pltpu.VMEM((2, 8, tall, tokens), BF16),
        pltpu.VMEM((8, tall, 2 * tokens), BF16),
        pltpu.VMEM((4 * tokens, ff), F32),
        pltpu.VMEM((2, tokens, ff), F32),
        pltpu.VMEM((tokens, ff), BF16),
        pltpu.VMEM((tokens, ff), BF16),
        pltpu.VMEM((3, 16, tokens), F32),
        pltpu.VMEM((7, 16, tokens), F32),
        pltpu.VMEM((1, tokens), F32),
        pltpu.VMEM((1, tokens), F32),
        pltpu.VMEM((1, tokens), jnp.int32),
        pltpu.VMEM((8, rows, ff), F32),
        *(
            pltpu.VMEM((*lead, rows, ff), BF16)
            for lead in ((), (2,), (), (), (2,), (), (2,), (), (), (2,))
        ),
        dma((7,)), dma((7,)), dma((7,)), dma((8,)), dma((8,)), dma((8,)), dma((8,)), dma((3,)), dma((3,)), dma((8,)), dma((8,)),
        dma((3,)), dma((3,)), dma((4,)), dma((4,)), dma((8,)), dma((8,)),
    ]
    outs = (
        jax.ShapeDtypeStruct((ff, tokens), BF16),
        jax.ShapeDtypeStruct((ff, tokens), BF16),
        jax.ShapeDtypeStruct((rows, ff), F32),
    )
    values = pl.pallas_call(
        functools.partial(kernel, rows, low),
        out_shape=tuple(pltpu.VMEM(o.shape, o.dtype) for o in outs),
        in_specs=[hbm, hbm, hbm, hbm, hbm, hbm, hbm, smem, smem],
        out_specs=(pl.BlockSpec(memory_space=pltpu.VMEM),) * 3,
        scratch_shapes=scratch,
        compiler_params=pltpu.CompilerParams(
            collective_id=0, has_side_effects=True, vmem_limit_bytes=60 * 1024 * 1024
        ),
    )(
        down_weight, grad_out.T, gate_pre.T, up_pre.T, line(new_logp), line(behav_logp), line(token_lag), lengths, versions
    )
    d_gate, d_up, d_down = pl.pallas_call(
        write_out,
        out_shape=outs,
        in_specs=[pl.BlockSpec(memory_space=pltpu.VMEM)] * 3,
        out_specs=(hbm, hbm, hbm),
        scratch_shapes=[dma((3,))],
    )(*(pltpu.with_memory_space_constraint(v, pltpu.VMEM) for v in values))
    return d_gate.T, d_up.T, d_down


def solution(mesh):
    split = Mesh(mesh.devices.reshape(4, 4, 2, mesh.shape["mp"]), (*DP, "mp"))
    placed = (P(DP, "mp"), P(DP, "mp"), P(DP, "mp"), P(DP, "mp"), P(DP), P(DP), P(DP), P(DP), P(DP))
    return jax.shard_map(
        local,
        mesh=split,
        in_specs=placed,
        out_specs=(P(DP, "mp"), P(DP, "mp"), P(DP, "mp")),
        check_vma=False,
    )
```

```python
import functools
import math

import jax
import jax.numpy as jnp
from jax import lax
from jax.experimental import pallas as pl
from jax.experimental.pallas import tpu as pltpu
from jax.sharding import Mesh
from jax.sharding import PartitionSpec as P

MAX_LAG = 5
DP = ("dp_0", "dp_1", "dp_2")
MESH = pl.DeviceIdType.MESH
F32, BF16 = jnp.float32, jnp.bfloat16
RATIO_CAP = 2.0
ROOT = math.sqrt(2.0 / math.pi)
CUBIC = 0.044715


def kernel(
    rows, low, weight, cotangent, gate, up, new_logp, old_logp, lag, length, version,
    gate_out, up_out, down_out,
    weights_all, cot_all, hidden, gate_v, up_v, act, up_slope, pool, others, far, acc, acc_in, sum_out, sum_in, hist_out, hist_in,
    new_v, old_v, lag_v, select, w_out, w_in, partial, a_out, b_out, c_out, d_out, e_out, a_in, b_in, c_in, d_in, e_in,
    copy_sem, hist_send, hist_recv, z_send, z_recv, ag_send, ag_recv, core_send, core_recv, swap_send, swap_recv,
    cross_send, cross_recv, far_send, far_recv, rs_send, rs_recv, w_send, w_recv,
):
    y, x, c, z = (lax.axis_index(name) for name in (*DP, "mp"))
    tokens, units = hidden.shape[0] // 4, hidden.shape[1]
    lo, hi = pl.ds(0, low), pl.ds(low, rows - low)
    side, column = x // 2, lax.rem(x, 2)

    def block(i, j):
        return lax.rem(y + 4 + j, 4) * 2 + lax.rem(column + i, 2)

    twin = (y, x, 1 - c, z)
    beside = (y, x + 1 - 2 * column, c, z)
    across = (y, 3 - x, c, z)
    ahead, behind = (lax.rem(y + 1, 4), x, c, z), (lax.rem(y + 3, 4), x, c, z)
    z_peers = {d: (y, x, c, lax.rem(z + 8 + d, 8)) for d in (-2, 2, -1, 1)}
    x_peers = [(y, lax.rem(x + d, 4), c, z) for d in range(1, 4)]
    y_peers = [(lax.rem(y + d, 4), x, c, z) for d in range(1, 4)]
    peers = [twin, *z_peers.values(), *x_peers, *y_peers]

    def remote(src, dst, send, recv, to):
        return pltpu.make_async_remote_copy(
            src_ref=src, dst_ref=dst, send_sem=send, recv_sem=recv, device_id=to, device_id_type=MESH
        )

    barrier = pltpu.get_barrier_semaphore()
    for peer in peers:
        pl.semaphore_signal(barrier, inc=1, device_id=peer, device_id_type=MESH)

    own = block(0, 0)
    local = [
        pltpu.make_async_copy(gate, gate_v, copy_sem.at[0]),
        pltpu.make_async_copy(up, up_v, copy_sem.at[1]),
        pltpu.make_async_copy(cotangent, cot_all.at[0], copy_sem.at[2]),
        pltpu.make_async_copy(weight, weights_all.at[own], copy_sem.at[3]),
    ]
    small = [
        pltpu.make_async_copy(src, dst, copy_sem.at[4 + n])
        for n, (src, dst) in enumerate(((lag, lag_v), (new_logp, new_v), (old_logp, old_v)))
    ]
    for copy in (*small, *local):
        copy.start()
    for copy in small:
        copy.wait()

    bins = lax.broadcasted_iota(jnp.int32, (16, tokens), 0)
    position = lax.broadcasted_iota(jnp.int32, (1, tokens), 1)
    live = position < length[0]
    token_version = lag_v[...] + version[0]
    match = jnp.where((token_version == bins) & live, 1.0, 0.0)
    counts = jnp.broadcast_to(jnp.sum(match, axis=1, keepdims=True), (16, tokens))
    hist_out[0] = counts

    local[0].wait()
    local[1].wait()

    def elementwise(start, size):
        here = pl.ds(start, size)
        v = gate_v[here].astype(F32)
        u = up_v[here].astype(F32)
        square = v * v
        t = jnp.tanh(ROOT * (v + CUBIC * (square * v)))
        half = 0.5 * (1.0 + t)
        a = v * half
        slope = half + (0.5 * v) * (1.0 - t * t) * (ROOT * (1.0 + (3.0 * CUBIC) * square))
        act[here] = a
        up_slope[here] = u * slope
        hidden[pl.ds(0, tokens), here] = (a * u).T.astype(BF16)

    def over_units(body, first, last):
        def step(n, carry):
            body(pl.multiple_of(n * 128, 128), 128)
            return carry

        lax.fori_loop(first, min(last, units // 128), step, 0)
        if last > units // 128 and units % 128:
            body(units // 128 * 128, units % 128)

    width = cotangent.shape[0]
    front, back = pl.ds(0, width // 2), pl.ds(width // 2, width // 2)

    tall = pool.shape[2]
    line = lax.broadcasted_iota(jnp.int32, (4 * tall, width), 0)
    source = lax.broadcasted_iota(jnp.int32, (4 * tall, width), 1)
    group = (line >= tall).astype(jnp.int32) + (line >= 2 * tall).astype(jnp.int32) + (line >= 3 * tall).astype(jnp.int32)
    row = line - tall * group
    parity = jnp.where(group < 2, c, 1 - c)
    wanted = rows * (2 * (group & 1) + parity) + row
    select[...] = jnp.where((source == wanted) & (row < rows), 1.0, 0.0).astype(BF16)

    chunks = pl.cdiv(units, 128)
    early = 4
    over_units(elementwise, 0, early)
    pl.semaphore_wait(barrier, len(peers))

    sent = []

    def go(copy):
        copy.start()
        sent.append(copy)

    for d in range(3):
        go(remote(hist_out.at[0], hist_in.at[d], hist_send.at[d], hist_recv.at[d], x_peers[d]))

    slots = {(1, 0): 0, (0, -1): 1, (0, 1): 2, (1, -1): 3, (1, 1): 4, (0, 2): 5, (1, 2): 7}

    def spread(i, j, to, as_i, as_j, half=0, part=None, src=None):
        view = weights_all.at[block(i, j)]
        view = view if part is None else view.at[part]
        sem = slots[(as_i, as_j)] + half
        go(remote(view if src is None else src, view, ag_send.at[sem], ag_recv.at[sem], to))

    def landed(i, j, half=0, part=None):
        view = weights_all.at[block(i, j)]
        view = view if part is None else view.at[part]
        sem = slots[(i, j)] + half
        remote(view, view, ag_send.at[sem], ag_recv.at[sem], twin).wait_recv()

    def z_wait(d, half=None):
        part = cot_all.at[d] if half is None else cot_all.at[d, (front, back)[half]]
        sem = d - 1 if half is None else (3, 7)[half]
        remote(part, part, z_send.at[0], z_recv.at[sem], twin).wait_recv()

    for n, (d, slot) in enumerate(((2, 2), (-2, 6), (1, 1), (-1, 7))):
        go(remote(cotangent, cot_all.at[slot], z_send.at[n], z_recv.at[slot - 1], z_peers[d]))
    spread(0, 0, beside, 1, 0, src=weight)
    spread(0, 0, ahead, 0, -1, src=weight)
    spread(0, 0, behind, 0, 1, src=weight)

    outgoing = lax.rem(z + side + 1, 2)

    def where(d):
        owner = lax.rem(z + 8 - d, 8)
        return lax.rem(owner, 2), owner // 2

    def swap(d):
        of, pair = where(d)
        pairs = pl.ds(pair * 2, 2)
        return remote(
            others.at[of, pairs], pool.at[of, pairs, :, pl.ds(tokens, tokens)], swap_send.at[d], swap_recv.at[d], twin
        )

    def place(d):
        of, pair = where(d)
        picked = jnp.dot(select[...], cot_all[d], preferred_element_type=F32)
        for k in range(2):
            pool[of, 2 * pair + k, :, pl.ds(0, tokens)] = picked[k * tall : (k + 1) * tall].astype(BF16)
            others[of, 2 * pair + k] = picked[(k + 2) * tall : (k + 3) * tall].astype(BF16)
        swap(d).start()

    def hand(pair):
        pairs = pl.ds(pair * 2, 2)
        return remote(pool.at[1 - side, pairs], far.at[pairs], far_send.at[pair], far_recv.at[pair], across)

    def export(d):
        swap(d).wait_recv()

        @pl.when(outgoing == d % 2)
        def _():
            hand(where(d)[1]).start()

    quarter = [pl.ds(n * tokens, tokens) for n in range(4)]
    first, second = pl.ds(0, early * 128), pl.ds(early * 128, units - early * 128)
    crossing = [
        remote(hidden.at[quarter[0], first], hidden.at[quarter[2], first], core_send.at[0], core_recv.at[0], across),
        remote(hidden.at[quarter[0], second], hidden.at[quarter[2], second], core_send.at[3], core_recv.at[3], across),
        remote(hidden.at[quarter[0]], hidden.at[quarter[1]], core_send.at[1], core_recv.at[1], twin),
        remote(hidden.at[quarter[2]], hidden.at[quarter[3]], core_send.at[2], core_recv.at[2], twin),
    ]
    crossing[0].start()
    local[2].wait()
    place(0)
    over_units(elementwise, early, chunks)
    crossing[1].start()
    crossing[2].start()
    export(0)

    def received(n):
        remote(hist_in.at[n], hist_in.at[n], hist_send.at[n], hist_recv.at[n], twin).wait_recv()
        return hist_in[n]

    counts = counts + received(0) + received(1) + received(2)
    hist_out[1] = counts
    for d in range(3):
        go(remote(hist_out.at[1], hist_in.at[3 + d], hist_send.at[3 + d], hist_recv.at[3 + d], y_peers[d]))

    z_wait(2)
    go(remote(cot_all.at[2], cot_all.at[3], z_send.at[4], z_recv.at[2], z_peers[1]))
    go(remote(cot_all.at[2, front], cot_all.at[4, front], z_send.at[5], z_recv.at[3], z_peers[2]))
    z_wait(6)
    go(remote(cot_all.at[6], cot_all.at[5], z_send.at[6], z_recv.at[4], z_peers[-1]))
    go(remote(cot_all.at[6, back], cot_all.at[4, back], z_send.at[7], z_recv.at[7], z_peers[-2]))

    landed(0, -1)
    spread(0, -1, ahead, 0, 2, 0, lo)
    landed(0, 1)
    spread(0, 1, behind, 0, 2, 1, hi)
    landed(1, 0)
    spread(1, 0, ahead, 1, -1)
    spread(1, 0, behind, 1, 1)
    counts = counts + received(3) + received(4) + received(5)
    hist_out[2] = counts
    go(remote(hist_out.at[2], hist_in.at[6], hist_send.at[6], hist_recv.at[6], twin))


    place(2)
    place(6)
    for d in (1, 7):
        z_wait(d)
        place(d)
    for d in (2, 6, 1, 7):
        export(d)
    landed(0, 2, 0, lo)
    landed(0, 2, 1, hi)
    spread(0, 2, beside, 1, 2)
    counts = counts + received(6)
    current = jnp.max(jnp.where(counts > 0, bins, -1), axis=0, keepdims=True)
    oldest = current - MAX_LAG
    valid_count = jnp.sum(jnp.where(bins >= oldest, counts, 0.0), axis=0, keepdims=True)
    valid = live & (token_version >= oldest)
    ratio = jnp.minimum(jnp.exp(new_v[...] - old_v[...]), RATIO_CAP)
    token_weight = jnp.where(valid, ratio, 0.0) * (32.0 / valid_count)

    w_out[...] = jnp.broadcast_to(token_weight, w_out.shape)
    weighing = [
        remote(w_out, w_in.at[0], w_send.at[0], w_recv.at[0], twin),
        remote(w_out, w_in.at[1], w_send.at[1], w_recv.at[1], across),
        remote(w_in.at[1], w_in.at[2], w_send.at[2], w_recv.at[2], twin),
    ]
    weighing[0].start()
    weighing[1].start()
    for d in (3, 5):
        z_wait(d)
        place(d)
    for d in (3, 5):
        export(d)
    weighing[1].wait_recv()
    weighing[2].start()
    z_wait(4, 0)
    z_wait(4, 1)
    place(4)
    export(4)
    crossing[0].wait_recv()
    crossing[1].wait_recv()
    crossing[3].start()
    weighing[0].wait_recv()
    weighing[2].wait_recv()

    def scale(view, left, right):
        def step(n, carry):
            for k, row in enumerate((left, right)):
                here = pl.ds(k * tokens, tokens)
                view[n, :, here] = (row * view[n, :, here].astype(F32)).astype(BF16)
            return carry

        lax.fori_loop(0, 8, step, 0)

    scale(pool.at[side], token_weight, w_in[0, 0:1])
    near_rows, far_rows = pl.ds(0, 2 * tokens), pl.ds(2 * tokens, 2 * tokens)

    def accumulate(group, first):
        for source, here in ((pool.at[side], near_rows), (far, far_rows)):
            total = None if first else acc[here]
            for i, j in group:
                p = block(i, j)
                term = lax.dot_general(
                    source[p, pl.ds(0, rows)], weights_all[p], (((0,), (0,)), ((), ())), preferred_element_type=F32
                )
                total = term if total is None else total + term
            acc[here] = total

    crossing[2].wait_recv()
    for pair in range(4):
        hand(pair).wait_recv()
    scale(far, w_in[1, 0:1], w_in[2, 0:1])
    crossing[3].wait_recv()

    def product(n, i, j):
        p = lax.rem(y + 4 + j, 4) * 2 + lax.rem(column + i, 2)
        near = jnp.dot(pool[side, p], hidden[near_rows], preferred_element_type=F32)
        partial[n] = (near + jnp.dot(far[p], hidden[far_rows], preferred_element_type=F32))[:rows]

    def shift(n):
        i = jnp.where((n < 3) | (n == 6), 1, 0)
        j = jnp.where((n == 0) | (n == 5), 2, jnp.where((n == 1) | (n == 3), 1, jnp.where((n == 2) | (n == 4), 3, 0)))
        return i, j

    def products(first, last):
        def step(n, carry):
            product(n, *shift(n))
            return carry

        lax.fori_loop(first, last, step, 0)

    sums = {
        "a": (a_out, a_in, 0, beside),
        "b0": (b_out.at[0], b_in.at[0], 1, ahead),
        "b1": (b_out.at[1], b_in.at[1], 2, behind),
        "c0": (c_out.at[lo], c_in.at[lo], 3, ahead),
        "c1": (c_out.at[hi], c_in.at[hi], 4, behind),
        "d": (d_out, d_in, 5, beside),
        "e0": (e_out.at[0, lo], e_in.at[0, lo], 6, ahead),
        "e1": (e_out.at[1, hi], e_in.at[1, hi], 7, behind),
        "f0": (e_out.at[0, hi], e_in.at[0, hi], 8, ahead),
        "f1": (e_out.at[1, lo], e_in.at[1, lo], 9, behind),
    }
    sums = {key: remote(src, dst, rs_send.at[n], rs_recv.at[n], to) for key, (src, dst, n, to) in sums.items()}

    products(0, 3)
    a_out[...] = partial[0].astype(BF16)
    sums["a"].start()
    b_out[0] = partial[1].astype(BF16)
    sums["b0"].start()
    b_out[1] = partial[2].astype(BF16)
    sums["b1"].start()
    local[3].wait()
    accumulate(((0, 0), (1, 0), (0, -1), (0, 1)), True)
    landed(1, -1)
    landed(1, 1)
    landed(1, 2)
    accumulate(((1, -1), (1, 1), (0, 2), (1, 2)), False)
    swaps = [
        remote(acc.at[quarter[2 * n + 1]], acc_in.at[n], cross_send.at[n], cross_recv.at[n], twin) for n in range(2)
    ]
    swaps[1].start()
    swaps[0].start()
    products(3, 5)
    e_out[0, hi] = partial[3, hi].astype(BF16)
    sums["f0"].start()
    e_out[1, lo] = partial[4, lo].astype(BF16)
    sums["f1"].start()
    swaps[1].wait_recv()
    ff_parts = [pl.ds(0, 640), pl.ds(640, units - 640)]
    cross = []
    for n, part in enumerate(ff_parts):
        sum_out[:, part] = (acc[quarter[2], part] + acc_in[1, :, part]).astype(BF16)
        cross.append(
            remote(sum_out.at[:, part], sum_in.at[:, part], cross_send.at[2 + n], cross_recv.at[2 + n], across)
        )
        cross[-1].start()
    products(5, 8)
    sums["a"].wait_recv()
    c_out[...] = (partial[5] + a_in[...].astype(F32)).astype(BF16)
    sums["c0"].start()
    sums["c1"].start()
    sums["b0"].wait_recv()
    sums["b1"].wait_recv()
    d_out[...] = (partial[6] + b_in[0].astype(F32) + b_in[1].astype(F32)).astype(BF16)
    sums["d"].start()
    sums["c0"].wait_recv()
    e_out[0, lo] = (partial[3, lo] + c_in[lo].astype(F32)).astype(BF16)
    sums["e0"].start()
    sums["c1"].wait_recv()
    e_out[1, hi] = (partial[4, hi] + c_in[hi].astype(F32)).astype(BF16)
    sums["e1"].start()

    def finish(start, size):
        here = pl.ds(start, size)
        total = (acc[quarter[0], here] + acc_in[0, :, here] + sum_in[:, here].astype(F32)).T
        up_out[here] = (total * act[here]).astype(BF16)
        gate_out[here] = (total * up_slope[here]).astype(BF16)

    swaps[0].wait_recv()
    cross[0].wait_recv()
    over_units(finish, 0, 5)
    cross[1].wait_recv()
    over_units(finish, 5, chunks)
    sums["d"].wait_recv()
    down_out[...] = partial[7] + d_in[...].astype(F32)
    for key in ("f0", "f1", "e0", "e1"):
        sums[key].wait_recv()
    down_out[...] += e_in[0].astype(F32) + e_in[1].astype(F32)

    for copy in (*sent, *crossing, *weighing, *swaps, *cross, *sums.values()):
        copy.wait_send()
    for d in range(8):
        swap(d).wait_send()
    for pair in range(4):
        hand(pair).wait_send()


def write_out(*refs):
    sem = refs[-1]
    copies = [pltpu.make_async_copy(refs[n], refs[3 + n], sem.at[n]) for n in range(3)]
    for copy in copies:
        copy.start()
    for copy in copies:
        copy.wait()


def local(grad_out, gate_pre, up_pre, down_weight, new_logp, behav_logp, lengths, versions, token_lag):
    tokens, ff = gate_pre.shape
    rows = down_weight.shape[0]
    width = grad_out.shape[1]
    low, tall = 40, 88
    hbm = pl.BlockSpec(memory_space=pl.ANY)
    smem = pl.BlockSpec(memory_space=pltpu.SMEM)
    dma = pltpu.SemaphoreType.DMA

    def line(values):
        return values.reshape(1, tokens)

    scratch = [
        pltpu.VMEM((8, rows, ff), BF16),
        pltpu.VMEM((8, width, tokens), BF16),
        pltpu.VMEM((4 * tokens, ff), BF16),
        pltpu.VMEM((ff, tokens), BF16),
        pltpu.VMEM((ff, tokens), BF16),
        pltpu.VMEM((ff, tokens), F32),
        pltpu.VMEM((ff, tokens), F32),
        pltpu.VMEM((2, 8, tall, 2 * tokens), BF16),
        pltpu.VMEM((2, 8, tall, tokens), BF16),
        pltpu.VMEM((8, tall, 2 * tokens), BF16),
        pltpu.VMEM((4 * tokens, ff), F32),
        pltpu.VMEM((2, tokens, ff), F32),
        pltpu.VMEM((tokens, ff), BF16),
        pltpu.VMEM((tokens, ff), BF16),
        pltpu.VMEM((3, 16, tokens), F32),
        pltpu.VMEM((7, 16, tokens), F32),
        pltpu.VMEM((1, tokens), F32),
        pltpu.VMEM((1, tokens), F32),
        pltpu.VMEM((1, tokens), jnp.int32),
        pltpu.VMEM((4 * tall, width), BF16),
        pltpu.VMEM((8, tokens), F32),
        pltpu.VMEM((3, 8, tokens), F32),
        pltpu.VMEM((8, rows, ff), F32),
        *(
            pltpu.VMEM((*lead, rows, ff), BF16)
            for lead in ((), (2,), (), (), (2,), (), (2,), (), (), (2,))
        ),
        dma((7,)), dma((7,)), dma((7,)), dma((8,)), dma((8,)), dma((8,)), dma((8,)), dma((4,)), dma((4,)), dma((8,)), dma((8,)),
        dma((4,)), dma((4,)), dma((4,)), dma((4,)), dma((10,)), dma((10,)), dma((3,)), dma((3,)),
    ]
    outs = (
        jax.ShapeDtypeStruct((ff, tokens), BF16),
        jax.ShapeDtypeStruct((ff, tokens), BF16),
        jax.ShapeDtypeStruct((rows, ff), F32),
    )
    values = pl.pallas_call(
        functools.partial(kernel, rows, low),
        out_shape=tuple(pltpu.VMEM(o.shape, o.dtype) for o in outs),
        in_specs=[hbm, hbm, hbm, hbm, hbm, hbm, hbm, smem, smem],
        out_specs=(pl.BlockSpec(memory_space=pltpu.VMEM),) * 3,
        scratch_shapes=scratch,
        compiler_params=pltpu.CompilerParams(
            collective_id=0, has_side_effects=True, vmem_limit_bytes=60 * 1024 * 1024
        ),
    )(
        down_weight, grad_out.T, gate_pre.T, up_pre.T, line(new_logp), line(behav_logp), line(token_lag), lengths, versions
    )
    d_gate, d_up, d_down = pl.pallas_call(
        write_out,
        out_shape=outs,
        in_specs=[pl.BlockSpec(memory_space=pltpu.VMEM)] * 3,
        out_specs=(hbm, hbm, hbm),
        scratch_shapes=[dma((3,))],
    )(*(pltpu.with_memory_space_constraint(v, pltpu.VMEM) for v in values))
    return d_gate.T, d_up.T, d_down


def solution(mesh):
    split = Mesh(mesh.devices.reshape(4, 4, 2, mesh.shape["mp"]), (*DP, "mp"))
    placed = (P(DP, "mp"), P(DP, "mp"), P(DP, "mp"), P(DP, "mp"), P(DP), P(DP), P(DP), P(DP), P(DP))
    return jax.shard_map(
        local,
        mesh=split,
        in_specs=placed,
        out_specs=(P(DP, "mp"), P(DP, "mp"), P(DP, "mp")),
        check_vma=False,
    )
```

```python
import functools
import math

import jax
import jax.numpy as jnp
from jax import lax
from jax.experimental import pallas as pl
from jax.experimental.pallas import tpu as pltpu
from jax.sharding import Mesh
from jax.sharding import PartitionSpec as P

MAX_LAG = 5
DP = ("dp_0", "dp_1", "dp_2")
MESH = pl.DeviceIdType.MESH
F32, BF16 = jnp.float32, jnp.bfloat16
RATIO_CAP = 2.0
ROOT = math.sqrt(2.0 / math.pi)
CUBIC = 0.044715


def kernel(
    rows, low, weight, cotangent, gate, up, new_logp, old_logp, lag, length, version,
    gate_out, up_out, down_out,
    weights_all, cot_all, hidden, gate_v, up_v, act, up_slope, pool, others, far, acc, acc_in, sum_out, sum_in, hist_out, hist_in,
    new_v, old_v, lag_v, select, w_out, w_in, partial, a_out, b_out, c_out, d_out, e_out, a_in, b_in, c_in, d_in, e_in,
    copy_sem, hist_send, hist_recv, z_send, z_recv, ag_send, ag_recv, core_send, core_recv, swap_send, swap_recv,
    cross_send, cross_recv, far_send, far_recv, rs_send, rs_recv, w_send, w_recv,
):
    y, x, c, z = (lax.axis_index(name) for name in (*DP, "mp"))
    tokens, units = hidden.shape[0] // 4, hidden.shape[1]
    lo, hi = pl.ds(0, low), pl.ds(low, rows - low)
    side, column = x // 2, lax.rem(x, 2)

    def block(i, j):
        return lax.rem(y + 4 + j, 4) * 2 + lax.rem(column + i, 2)

    twin = (y, x, 1 - c, z)
    beside = (y, x + 1 - 2 * column, c, z)
    across = (y, 3 - x, c, z)
    ahead, behind = (lax.rem(y + 1, 4), x, c, z), (lax.rem(y + 3, 4), x, c, z)
    z_peers = {d: (y, x, c, lax.rem(z + 8 + d, 8)) for d in (-2, 2, -1, 1)}
    x_peers = [(y, lax.rem(x + d, 4), c, z) for d in range(1, 4)]
    y_peers = [(lax.rem(y + d, 4), x, c, z) for d in range(1, 4)]
    peers = [twin, *z_peers.values(), *x_peers, *y_peers]

    def remote(src, dst, send, recv, to):
        return pltpu.make_async_remote_copy(
            src_ref=src, dst_ref=dst, send_sem=send, recv_sem=recv, device_id=to, device_id_type=MESH
        )

    barrier = pltpu.get_barrier_semaphore()
    for peer in peers:
        pl.semaphore_signal(barrier, inc=1, device_id=peer, device_id_type=MESH)

    own = block(0, 0)
    local = [
        pltpu.make_async_copy(gate, gate_v, copy_sem.at[0]),
        pltpu.make_async_copy(up, up_v, copy_sem.at[1]),
        pltpu.make_async_copy(cotangent, cot_all.at[0], copy_sem.at[2]),
        pltpu.make_async_copy(weight, weights_all.at[own], copy_sem.at[3]),
    ]
    small = [
        pltpu.make_async_copy(src, dst, copy_sem.at[4 + n])
        for n, (src, dst) in enumerate(((lag, lag_v), (new_logp, new_v), (old_logp, old_v)))
    ]
    for copy in (*small, *local):
        copy.start()
    for copy in small:
        copy.wait()

    bins = lax.broadcasted_iota(jnp.int32, (16, tokens), 0)
    position = lax.broadcasted_iota(jnp.int32, (1, tokens), 1)
    live = position < length[0]
    token_version = lag_v[...] + version[0]
    match = jnp.where((token_version == bins) & live, 1.0, 0.0)
    counts = jnp.broadcast_to(jnp.sum(match, axis=1, keepdims=True), (16, tokens))
    hist_out[0] = counts

    local[0].wait()
    local[1].wait()

    def elementwise(start, size):
        here = pl.ds(start, size)
        v = gate_v[here].astype(F32)
        u = up_v[here].astype(F32)
        square = v * v
        t = jnp.tanh(ROOT * (v + CUBIC * (square * v)))
        half = 0.5 * (1.0 + t)
        a = v * half
        slope = half + (0.5 * v) * (1.0 - t * t) * (ROOT * (1.0 + (3.0 * CUBIC) * square))
        act[here] = a
        up_slope[here] = u * slope
        hidden[pl.ds(0, tokens), here] = (a * u).T.astype(BF16)

    def over_units(body, first, last):
        def step(n, carry):
            body(pl.multiple_of(n * 128, 128), 128)
            return carry

        lax.fori_loop(first, min(last, units // 128), step, 0)
        if last > units // 128 and units % 128:
            body(units // 128 * 128, units % 128)

    width = cotangent.shape[0]
    front, back = pl.ds(0, width // 2), pl.ds(width // 2, width // 2)

    tall = pool.shape[2]
    line = lax.broadcasted_iota(jnp.int32, (4 * tall, width), 0)
    source = lax.broadcasted_iota(jnp.int32, (4 * tall, width), 1)
    group = (line >= tall).astype(jnp.int32) + (line >= 2 * tall).astype(jnp.int32) + (line >= 3 * tall).astype(jnp.int32)
    row = line - tall * group
    parity = jnp.where(group < 2, c, 1 - c)
    wanted = rows * (2 * (group & 1) + parity) + row
    select[...] = jnp.where((source == wanted) & (row < rows), 1.0, 0.0).astype(BF16)

    chunks = pl.cdiv(units, 128)
    early = 4
    over_units(elementwise, 0, early)
    pl.semaphore_wait(barrier, len(peers))

    sent = []

    def go(copy):
        copy.start()
        sent.append(copy)

    for d in range(3):
        go(remote(hist_out.at[0], hist_in.at[d], hist_send.at[d], hist_recv.at[d], x_peers[d]))

    slots = {(1, 0): 0, (0, -1): 1, (0, 1): 2, (1, -1): 3, (1, 1): 4, (0, 2): 5, (1, 2): 7}

    def spread(i, j, to, as_i, as_j, half=0, part=None, src=None):
        view = weights_all.at[block(i, j)]
        view = view if part is None else view.at[part]
        sem = slots[(as_i, as_j)] + half
        go(remote(view if src is None else src, view, ag_send.at[sem], ag_recv.at[sem], to))

    def landed(i, j, half=0, part=None):
        view = weights_all.at[block(i, j)]
        view = view if part is None else view.at[part]
        sem = slots[(i, j)] + half
        remote(view, view, ag_send.at[sem], ag_recv.at[sem], twin).wait_recv()

    def z_wait(d, half=None):
        part = cot_all.at[d] if half is None else cot_all.at[d, (front, back)[half]]
        sem = d - 1 if half is None else (3, 7)[half]
        remote(part, part, z_send.at[0], z_recv.at[sem], twin).wait_recv()

    for n, (d, slot) in enumerate(((2, 2), (-2, 6), (1, 1), (-1, 7))):
        go(remote(cotangent, cot_all.at[slot], z_send.at[n], z_recv.at[slot - 1], z_peers[d]))
    spread(0, 0, beside, 1, 0, src=weight)
    spread(0, 0, ahead, 0, -1, src=weight)
    spread(0, 0, behind, 0, 1, src=weight)

    outgoing = lax.rem(z + side + 1, 2)

    def where(d):
        owner = lax.rem(z + 8 - d, 8)
        return lax.rem(owner, 2), owner // 2

    def swap(d):
        of, pair = where(d)
        pairs = pl.ds(pair * 2, 2)
        return remote(
            others.at[of, pairs], pool.at[of, pairs, :, pl.ds(tokens, tokens)], swap_send.at[d], swap_recv.at[d], twin
        )

    def place(d):
        of, pair = where(d)
        picked = jnp.dot(select[...], cot_all[d], preferred_element_type=F32)
        for k in range(2):
            pool[of, 2 * pair + k, :, pl.ds(0, tokens)] = picked[k * tall : (k + 1) * tall].astype(BF16)
            others[of, 2 * pair + k] = picked[(k + 2) * tall : (k + 3) * tall].astype(BF16)
        swap(d).start()

    def hand(pair):
        pairs = pl.ds(pair * 2, 2)
        return remote(pool.at[1 - side, pairs], far.at[pairs], far_send.at[pair], far_recv.at[pair], across)

    def export(d):
        swap(d).wait_recv()

        @pl.when(outgoing == d % 2)
        def _():
            hand(where(d)[1]).start()

    quarter = [pl.ds(n * tokens, tokens) for n in range(4)]
    first, second = pl.ds(0, early * 128), pl.ds(early * 128, units - early * 128)
    crossing = [
        remote(hidden.at[quarter[0], first], hidden.at[quarter[2], first], core_send.at[0], core_recv.at[0], across),
        remote(hidden.at[quarter[0], second], hidden.at[quarter[2], second], core_send.at[3], core_recv.at[3], across),
        remote(hidden.at[quarter[0]], hidden.at[quarter[1]], core_send.at[1], core_recv.at[1], twin),
        remote(hidden.at[quarter[2]], hidden.at[quarter[3]], core_send.at[2], core_recv.at[2], twin),
    ]
    crossing[0].start()
    local[2].wait()
    place(0)
    over_units(elementwise, early, chunks)
    crossing[1].start()
    crossing[2].start()
    export(0)

    def received(n):
        remote(hist_in.at[n], hist_in.at[n], hist_send.at[n], hist_recv.at[n], twin).wait_recv()
        return hist_in[n]

    counts = counts + received(0) + received(1) + received(2)
    hist_out[1] = counts
    for d in range(3):
        go(remote(hist_out.at[1], hist_in.at[3 + d], hist_send.at[3 + d], hist_recv.at[3 + d], y_peers[d]))

    z_wait(2)
    go(remote(cot_all.at[2], cot_all.at[3], z_send.at[4], z_recv.at[2], z_peers[1]))
    go(remote(cot_all.at[2, front], cot_all.at[4, front], z_send.at[5], z_recv.at[3], z_peers[2]))
    z_wait(6)
    go(remote(cot_all.at[6], cot_all.at[5], z_send.at[6], z_recv.at[4], z_peers[-1]))
    go(remote(cot_all.at[6, back], cot_all.at[4, back], z_send.at[7], z_recv.at[7], z_peers[-2]))

    landed(0, -1)
    spread(0, -1, ahead, 0, 2, 0, lo)
    landed(0, 1)
    spread(0, 1, behind, 0, 2, 1, hi)
    landed(1, 0)
    spread(1, 0, ahead, 1, -1)
    spread(1, 0, behind, 1, 1)
    counts = counts + received(3) + received(4) + received(5)
    hist_out[2] = counts
    go(remote(hist_out.at[2], hist_in.at[6], hist_send.at[6], hist_recv.at[6], twin))


    place(2)
    place(6)
    for d in (1, 7):
        z_wait(d)
        place(d)
    for d in (2, 6, 1, 7):
        export(d)
    landed(0, 2, 0, lo)
    landed(0, 2, 1, hi)
    spread(0, 2, beside, 1, 2)
    counts = counts + received(6)
    current = jnp.max(jnp.where(counts > 0, bins, -1), axis=0, keepdims=True)
    oldest = current - MAX_LAG
    valid_count = jnp.sum(jnp.where(bins >= oldest, counts, 0.0), axis=0, keepdims=True)
    valid = live & (token_version >= oldest)
    ratio = jnp.minimum(jnp.exp(new_v[...] - old_v[...]), RATIO_CAP)
    token_weight = jnp.where(valid, ratio, 0.0) * (32.0 / valid_count)

    w_out[...] = jnp.broadcast_to(token_weight, w_out.shape)
    weighing = [
        remote(w_out, w_in.at[0], w_send.at[0], w_recv.at[0], twin),
        remote(w_out, w_in.at[1], w_send.at[1], w_recv.at[1], across),
        remote(w_in.at[1], w_in.at[2], w_send.at[2], w_recv.at[2], twin),
    ]
    weighing[0].start()
    weighing[1].start()
    for d in (3, 5):
        z_wait(d)
        place(d)
    for d in (3, 5):
        export(d)
    weighing[1].wait_recv()
    weighing[2].start()
    z_wait(4, 0)
    z_wait(4, 1)
    place(4)
    export(4)
    crossing[0].wait_recv()
    crossing[1].wait_recv()
    crossing[3].start()
    weighing[0].wait_recv()
    weighing[2].wait_recv()

    def scale(view, left, right):
        def step(n, carry):
            for k, row in enumerate((left, right)):
                here = pl.ds(k * tokens, tokens)
                view[n, :, here] = (row * view[n, :, here].astype(F32)).astype(BF16)
            return carry

        lax.fori_loop(0, 8, step, 0)

    scale(pool.at[side], token_weight, w_in[0, 0:1])
    near_rows, far_rows = pl.ds(0, 2 * tokens), pl.ds(2 * tokens, 2 * tokens)

    def accumulate(group, first):
        for source, here in ((pool.at[side], near_rows), (far, far_rows)):
            total = None if first else acc[here]
            for i, j in group:
                p = block(i, j)
                term = lax.dot_general(
                    source[p, pl.ds(0, rows)], weights_all[p], (((0,), (0,)), ((), ())), preferred_element_type=F32
                )
                total = term if total is None else total + term
            acc[here] = total

    crossing[2].wait_recv()
    for pair in range(4):
        hand(pair).wait_recv()
    scale(far, w_in[1, 0:1], w_in[2, 0:1])
    crossing[3].wait_recv()

    def product(n, i, j):
        p = lax.rem(y + 4 + j, 4) * 2 + lax.rem(column + i, 2)
        near = jnp.dot(pool[side, p], hidden[near_rows], preferred_element_type=F32)
        partial[n] = (near + jnp.dot(far[p], hidden[far_rows], preferred_element_type=F32))[:rows]

    def shift(n):
        i = jnp.where((n < 3) | (n == 6), 1, 0)
        j = jnp.where((n == 0) | (n == 5), 2, jnp.where((n == 1) | (n == 3), 1, jnp.where((n == 2) | (n == 4), 3, 0)))
        return i, j

    def products(first, last):
        def step(n, carry):
            product(n, *shift(n))
            return carry

        lax.fori_loop(first, last, step, 0)

    sums = {
        "a": (a_out, a_in, 0, beside),
        "b0": (b_out.at[0], b_in.at[0], 1, ahead),
        "b1": (b_out.at[1], b_in.at[1], 2, behind),
        "c0": (c_out.at[lo], c_in.at[lo], 3, ahead),
        "c1": (c_out.at[hi], c_in.at[hi], 4, behind),
        "d": (d_out, d_in, 5, beside),
        "e0": (e_out.at[0, lo], e_in.at[0, lo], 6, ahead),
        "e1": (e_out.at[1, hi], e_in.at[1, hi], 7, behind),
        "f0": (e_out.at[0, hi], e_in.at[0, hi], 8, ahead),
        "f1": (e_out.at[1, lo], e_in.at[1, lo], 9, behind),
    }
    sums = {key: remote(src, dst, rs_send.at[n], rs_recv.at[n], to) for key, (src, dst, n, to) in sums.items()}

    products(0, 3)
    a_out[...] = partial[0].astype(BF16)
    sums["a"].start()
    b_out[0] = partial[1].astype(BF16)
    sums["b0"].start()
    b_out[1] = partial[2].astype(BF16)
    sums["b1"].start()
    local[3].wait()
    accumulate(((0, 0), (1, 0), (0, -1), (0, 1)), True)
    landed(1, -1)
    landed(1, 1)
    landed(1, 2)
    accumulate(((1, -1), (1, 1), (0, 2), (1, 2)), False)
    swaps = [
        remote(acc.at[quarter[2 * n + 1]], acc_in.at[n], cross_send.at[n], cross_recv.at[n], twin) for n in range(2)
    ]
    swaps[1].start()
    swaps[0].start()
    products(3, 5)
    e_out[0, hi] = partial[3, hi].astype(BF16)
    sums["f0"].start()
    e_out[1, lo] = partial[4, lo].astype(BF16)
    sums["f1"].start()
    swaps[1].wait_recv()
    ff_parts = [pl.ds(0, 640), pl.ds(640, units - 640)]
    cross = []
    for n, part in enumerate(ff_parts):
        sum_out[:, part] = (acc[quarter[2], part] + acc_in[1, :, part]).astype(BF16)
        cross.append(
            remote(sum_out.at[:, part], sum_in.at[:, part], cross_send.at[2 + n], cross_recv.at[2 + n], across)
        )
        cross[-1].start()
    products(5, 8)
    sums["a"].wait_recv()
    c_out[...] = (partial[5] + a_in[...].astype(F32)).astype(BF16)
    sums["c0"].start()
    sums["c1"].start()
    sums["b0"].wait_recv()
    sums["b1"].wait_recv()
    d_out[...] = (partial[6] + b_in[0].astype(F32) + b_in[1].astype(F32)).astype(BF16)
    sums["d"].start()
    sums["c0"].wait_recv()
    e_out[0, lo] = (partial[3, lo] + c_in[lo].astype(F32)).astype(BF16)
    sums["e0"].start()
    sums["c1"].wait_recv()
    e_out[1, hi] = (partial[4, hi] + c_in[hi].astype(F32)).astype(BF16)
    sums["e1"].start()

    def finish(start, size):
        here = pl.ds(start, size)
        total = (acc[quarter[0], here] + acc_in[0, :, here] + sum_in[:, here].astype(F32)).T
        up_out[here] = (total * act[here]).astype(BF16)
        gate_out[here] = (total * up_slope[here]).astype(BF16)

    sums["d"].wait_recv()
    down_out[...] = partial[7] + d_in[...].astype(F32)
    swaps[0].wait_recv()
    cross[0].wait_recv()
    over_units(finish, 0, 5)
    cross[1].wait_recv()
    over_units(finish, 5, chunks)
    for key in ("f0", "f1", "e0", "e1"):
        sums[key].wait_recv()
    down_out[...] += e_in[0].astype(F32) + e_in[1].astype(F32)

    for copy in (*sent, *crossing, *weighing, *swaps, *cross, *sums.values()):
        copy.wait_send()
    for d in range(8):
        swap(d).wait_send()
    for pair in range(4):
        hand(pair).wait_send()


def write_out(*refs):
    sem = refs[-1]
    copies = [pltpu.make_async_copy(refs[n], refs[3 + n], sem.at[n]) for n in range(3)]
    for copy in copies:
        copy.start()
    for copy in copies:
        copy.wait()


def local(grad_out, gate_pre, up_pre, down_weight, new_logp, behav_logp, lengths, versions, token_lag):
    tokens, ff = gate_pre.shape
    rows = down_weight.shape[0]
    width = grad_out.shape[1]
    low, tall = 40, 88
    hbm = pl.BlockSpec(memory_space=pl.ANY)
    smem = pl.BlockSpec(memory_space=pltpu.SMEM)
    dma = pltpu.SemaphoreType.DMA

    def line(values):
        return values.reshape(1, tokens)

    scratch = [
        pltpu.VMEM((8, rows, ff), BF16),
        pltpu.VMEM((8, width, tokens), BF16),
        pltpu.VMEM((4 * tokens, ff), BF16),
        pltpu.VMEM((ff, tokens), BF16),
        pltpu.VMEM((ff, tokens), BF16),
        pltpu.VMEM((ff, tokens), F32),
        pltpu.VMEM((ff, tokens), F32),
        pltpu.VMEM((2, 8, tall, 2 * tokens), BF16),
        pltpu.VMEM((2, 8, tall, tokens), BF16),
        pltpu.VMEM((8, tall, 2 * tokens), BF16),
        pltpu.VMEM((4 * tokens, ff), F32),
        pltpu.VMEM((2, tokens, ff), F32),
        pltpu.VMEM((tokens, ff), BF16),
        pltpu.VMEM((tokens, ff), BF16),
        pltpu.VMEM((3, 16, tokens), F32),
        pltpu.VMEM((7, 16, tokens), F32),
        pltpu.VMEM((1, tokens), F32),
        pltpu.VMEM((1, tokens), F32),
        pltpu.VMEM((1, tokens), jnp.int32),
        pltpu.VMEM((4 * tall, width), BF16),
        pltpu.VMEM((8, tokens), F32),
        pltpu.VMEM((3, 8, tokens), F32),
        pltpu.VMEM((8, rows, ff), F32),
        *(
            pltpu.VMEM((*lead, rows, ff), BF16)
            for lead in ((), (2,), (), (), (2,), (), (2,), (), (), (2,))
        ),
        dma((7,)), dma((7,)), dma((7,)), dma((8,)), dma((8,)), dma((8,)), dma((8,)), dma((4,)), dma((4,)), dma((8,)), dma((8,)),
        dma((4,)), dma((4,)), dma((4,)), dma((4,)), dma((10,)), dma((10,)), dma((3,)), dma((3,)),
    ]
    outs = (
        jax.ShapeDtypeStruct((ff, tokens), BF16),
        jax.ShapeDtypeStruct((ff, tokens), BF16),
        jax.ShapeDtypeStruct((rows, ff), F32),
    )
    values = pl.pallas_call(
        functools.partial(kernel, rows, low),
        out_shape=tuple(pltpu.VMEM(o.shape, o.dtype) for o in outs),
        in_specs=[hbm, hbm, hbm, hbm, hbm, hbm, hbm, smem, smem],
        out_specs=(pl.BlockSpec(memory_space=pltpu.VMEM),) * 3,
        scratch_shapes=scratch,
        compiler_params=pltpu.CompilerParams(
            collective_id=0, has_side_effects=True, vmem_limit_bytes=60 * 1024 * 1024
        ),
    )(
        down_weight, grad_out.T, gate_pre.T, up_pre.T, line(new_logp), line(behav_logp), line(token_lag), lengths, versions
    )
    d_gate, d_up, d_down = pl.pallas_call(
        write_out,
        out_shape=outs,
        in_specs=[pl.BlockSpec(memory_space=pltpu.VMEM)] * 3,
        out_specs=(hbm, hbm, hbm),
        scratch_shapes=[dma((3,))],
    )(*(pltpu.with_memory_space_constraint(v, pltpu.VMEM) for v in values))
    return d_gate.T, d_up.T, d_down


def solution(mesh):
    split = Mesh(mesh.devices.reshape(4, 4, 2, mesh.shape["mp"]), (*DP, "mp"))
    placed = (P(DP, "mp"), P(DP, "mp"), P(DP, "mp"), P(DP, "mp"), P(DP), P(DP), P(DP), P(DP), P(DP))
    return jax.shard_map(
        local,
        mesh=split,
        in_specs=placed,
        out_specs=(P(DP, "mp"), P(DP, "mp"), P(DP, "mp")),
        check_vma=False,
    )
```
